8 devices in a mesh: dp: 2 (over y, z), ep: 4 (over x, core).
Axes of the slice: x: 2, y: 2, z: 1, core: 2. Of those that a mesh axis runs over, the one named last changes fastest.
Arguments:
- x: bfloat16 [2, 4, 256, 7168], P('dp', 'ep'), parts along dimension 0
- expert: int32 [2, 4, 256, 8], P('dp', 'ep'), parts along dimension 0
- slot: int32 [2, 4, 256, 8], P('dp', 'ep'), parts along dimension 0
- gate: float32 [2, 4, 256, 8], P('dp', 'ep'), parts along dimension 0
- w_gate: bfloat16 [24, 7168, 2048], P('ep')
- w_up: bfloat16 [24, 7168, 2048], P('ep')
- w_down: bfloat16 [24, 2048, 7168], P('ep')
- s_gate: bfloat16 [7168, 2048], replicated
- s_up: bfloat16 [7168, 2048], replicated
- s_down: bfloat16 [2048, 7168], replicated
Outputs:
- y: bfloat16 [2, 4, 256, 7168], P('dp', 'ep'), parts along dimension 0
There are 2 independent parts. The reference program is written for one: setup_inputs(seed, part) draws one part's arguments, and reference() takes and returns one part's arrays. A program takes and returns all parts, laid end to end along the dimension named above; an argument that names none is the same for every part.
All inputs are finite; a program needn't handle non-finite values.
Results may differ from the reference program's by a relative error of at most 0.009.
Values are sent between devices in bfloat16 or wider.
A program may use at most 2 GiB of HBM per device.

```python
import jax
import jax.numpy as jnp

MEMBERS = 4
TOKENS = 256
D = 7168
FF = 2048
TOP = 8
EXPERTS = 24
SHARED_FF = 2048
SLOTS = 5 * TOKENS * TOP // (4 * EXPERTS)


def setup_inputs(seed: int = 0, part: int = 0) -> dict:
    own, k1, k2, k3, k4, k5, k6 = jax.random.split(jax.random.key(seed), 7)
    kx, ke, kl, kg = jax.random.split(jax.random.fold_in(own, part), 4)
    devices = (1, MEMBERS)
    place = jax.random.permutation(kl, jnp.arange(EXPERTS, dtype=jnp.uint32))
    slow = ((EXPERTS + (9 * place) % EXPERTS) << ((9 * place) // EXPERTS)) // EXPERTS
    wait = (jax.random.bits(ke, (*devices, TOKENS, EXPERTS), jnp.uint32) >> 10) * slow
    expert = jnp.argsort(wait, axis=-1)[..., :TOP].astype(jnp.int32)
    chosen = jax.nn.one_hot(expert, EXPERTS, dtype=jnp.int32)
    in_line = jnp.cumsum(chosen.reshape(*devices, TOKENS * TOP, EXPERTS), axis=2) - 1
    slot = jnp.sum(in_line.reshape(chosen.shape) * chosen, axis=-1)

    def one(key, rows, columns):
        return (jax.random.normal(key, (rows, columns), jnp.float32) * rows**-0.5).astype(jnp.bfloat16)

    def weights(key, rows, columns):
        return jax.lax.map(lambda k: one(k, rows, columns), jax.random.split(key, EXPERTS))

    return {
        "x": jax.random.normal(kx, (*devices, TOKENS, D), jnp.float32).astype(jnp.bfloat16),
        "expert": expert,
        "slot": slot,
        "gate": jax.nn.softmax(jax.random.normal(kg, expert.shape, jnp.float32)),
        "w_gate": weights(k1, D, FF),
        "w_up": weights(k2, D, FF),
        "w_down": weights(k3, FF, D),
        "s_gate": one(k4, D, SHARED_FF),
        "s_up": one(k5, D, SHARED_FF),
        "s_down": one(k6, SHARED_FF, D),
    }


def einsum(form, a, b):
    return jnp.einsum(form, a.astype(jnp.float32), b.astype(jnp.float32))


def for_all(x, s_gate, s_up, s_down):
    h = jax.nn.silu(einsum("...d,df->...f", x, s_gate)) * einsum("...d,df->...f", x, s_up)
    return einsum("...f,fd->...d", h.astype(jnp.bfloat16), s_down)


def reference(x, expert, slot, gate, w_gate, w_up, w_down, s_gate, s_up, s_down):
    to_expert = jax.nn.one_hot(expert, EXPERTS, dtype=jnp.bfloat16)
    to_slot = jax.nn.one_hot(slot, SLOTS, dtype=jnp.bfloat16)
    weighted = to_expert * gate[..., None].astype(jnp.bfloat16)
    dispatch = einsum("abtke,abtkc->abtec", to_expert, to_slot).astype(jnp.bfloat16)
    combine = einsum("abtke,abtkc->abtec", weighted, to_slot).astype(jnp.bfloat16)
    z = einsum("abtec,abtd->aebcd", dispatch, x).astype(jnp.bfloat16)
    h = jax.nn.silu(einsum("aebcd,edf->aebcf", z, w_gate))
    h = (h * einsum("aebcd,edf->aebcf", z, w_up)).astype(jnp.bfloat16)
    out = einsum("aebcf,efd->aebcd", h, w_down).astype(jnp.bfloat16)
    y = einsum("abtec,aebcd->abtd", combine, out)
    return (y + for_all(x, s_gate, s_up, s_down)).astype(jnp.bfloat16)
```

```python
import functools

import jax
import jax.numpy as jnp
from jax import lax
from jax.experimental import pallas as pl
from jax.experimental.pallas import tpu as pltpu
from jax.sharding import PartitionSpec as P

SAME = [(0, 1), (1, 0), (2, 3), (3, 2)]
CROSS = [(0, 2), (1, 3), (2, 0), (3, 1)]
STEP = 112
FIRST = 2048
CHUNKS = (1024, 3072, 3072)
VMEM = 62 * 2**20


def silu(g):
    return g / (1.0 + jnp.exp(-g))


def tables(expert, slot, gate, experts, slots):
    expert, slot, gate = expert.T, slot.T, gate.T
    hit = (expert[None] == jnp.arange(experts)[:, None, None]) & (slot < slots)[None]
    code = jnp.sum(jnp.where(hit, slot[None] + 1, 0), 1) - 1
    weight = jnp.sum(jnp.where(hit, gate[None], 0.0), 1)
    return jnp.stack([code.astype(jnp.float32), weight])


def up_kernel(depth, block, first, meta, code, x0, x1, x2, x3, wg, wu, *refs):
    if first:
        (g_out, u_out, z) = refs
    else:
        (g_in, u_in, h_out, z) = refs
    e, n = pl.program_id(0), pl.program_id(1)
    total = pl.multiple_of(meta[e * 8 + 4], 16)

    @pl.when(n == 0)
    def _():
        rows = lax.broadcasted_iota(jnp.int32, (STEP, 256), 0)
        for k, x in enumerate((x0, x1, x2, x3)):
            pick = (rows == code[0, k : k + 1, :]).astype(jnp.bfloat16)
            at = pl.multiple_of(meta[e * 8 + k], 16)

            @pl.loop(0, depth // 512)
            def _(c):
                cols = pl.ds(pl.multiple_of(c * 512, 512), 512)
                part = jnp.dot(pick, x[:, cols], preferred_element_type=jnp.float32)
                z[pl.ds(at, STEP), cols] = part.astype(jnp.bfloat16)

        z[pl.ds(total, STEP), :] = jnp.zeros((STEP, depth), jnp.bfloat16)

    size = (total + STEP - 1) // STEP
    for v in range(5):

        @pl.when(size == v)
        def _(v=v):
            m = v * STEP
            if v:
                g = jnp.dot(z[:m, :], wg[0], preferred_element_type=jnp.float32)
                u = jnp.dot(z[:m, :], wu[0], preferred_element_type=jnp.float32)
                if first:
                    g_out[0, :m, :] = g
                    u_out[0, :m, :] = u
                else:
                    g = g + g_in[0, :m, :]
                    u = u + u_in[0, :m, :]
                    h_out[0, :m, :] = (silu(g) * u).astype(jnp.bfloat16)
            if not first:
                h_out[0, m:, :] = jnp.zeros((5 * STEP - m, block), jnp.bfloat16)


def up(meta, code, xs, w_gate, w_up, start, block, partial=None):
    experts, _, ff = w_gate.shape
    depth = xs[0].shape[1]
    first = partial is None
    weight = pl.BlockSpec(
        (pl.Element(1), pl.Element(depth), pl.Element(block)),
        lambda e, n, m: (e, start, n * block),
    )
    whole = pl.BlockSpec((256, depth), lambda e, n, m: (0, 0), pipeline_mode=pl.Buffered(1))
    acc = pl.BlockSpec((1, 4 * STEP, block), lambda e, n, m: (e, 0, n))
    acc_shape = jax.ShapeDtypeStruct((experts, 4 * STEP, ff), jnp.float32)
    if first:
        out_shape, out_specs = [acc_shape] * 2, [acc] * 2
    else:
        out_shape = jax.ShapeDtypeStruct((experts, 5 * STEP, ff), jnp.bfloat16)
        out_specs = pl.BlockSpec((1, 5 * STEP, block), lambda e, n, m: (e, 0, n))
    return pl.pallas_call(
        functools.partial(up_kernel, depth, block, first),
        grid_spec=pltpu.PrefetchScalarGridSpec(
            num_scalar_prefetch=1,
            grid=(experts, ff // block),
            in_specs=[pl.BlockSpec((1, 4, 256), lambda e, n, m: (e, 0, 0))]
            + [whole] * 4
            + [weight] * 2
            + ([] if first else [acc] * 2),
            out_specs=out_specs,
            scratch_shapes=[pltpu.VMEM((5 * STEP, depth), jnp.bfloat16)],
        ),
        out_shape=out_shape,
        compiler_params=pltpu.CompilerParams(
            vmem_limit_bytes=VMEM, dimension_semantics=("arbitrary", "arbitrary")
        ),
        cost_estimate=pl.CostEstimate(
            flops=experts * 300 * depth * ff * 4,
            bytes_accessed=experts * depth * ff * 4,
            transcendentals=0,
        ),
        name="up_first" if first else "up_rest",
    )(meta, code, *xs, w_gate, w_up, *(() if first else partial))


def down_kernel(experts, block, meta, code, gate, h, wd, own, far, near, wt, tmp, stack):
    @pl.when(pl.program_id(0) == 0)
    def _():
        tmp[...] = jnp.zeros_like(tmp)
        rows = lax.broadcasted_iota(jnp.int32, (STEP, 256), 0)
        for k in range(4):
            for e in range(experts):
                hit = rows == code[e, k : k + 1, :]
                wt[k, e * STEP : (e + 1) * STEP, :] = jnp.where(
                    hit, gate[e, k : k + 1, :], 0.0
                ).astype(jnp.bfloat16)

    @pl.loop(0, experts)
    def _(e):
        total = meta[e * 8 + 4]
        size = (total + STEP - 1) // STEP
        for v in range(1, 5):

            @pl.when(size == v)
            def _(v=v):
                m = v * STEP
                out = jnp.dot(h[e, :m, :], wd[e], preferred_element_type=jnp.float32)
                tmp[:m, :] = out.astype(jnp.bfloat16)

        to = pl.ds(pl.multiple_of(e * STEP, STEP), STEP)
        for k in range(4):
            at = pl.multiple_of(meta[e * 8 + k], 16)
            stack[k, to, :] = tmp[pl.ds(at, STEP), :]

    def summed(k):
        return lax.dot_general(
            wt[k], stack[k], (((0,), (0,)), ((), ())), preferred_element_type=jnp.float32
        )

    own[...] = summed(0)
    far[...] = summed(2)
    near[0] = summed(1).astype(jnp.bfloat16)
    near[1] = summed(3).astype(jnp.bfloat16)


def down(meta, code, gate, h, w_down, start, columns, block):
    experts, ff, _ = w_down.shape
    once = pl.Buffered(1)
    return pl.pallas_call(
        functools.partial(down_kernel, experts, block),
        grid_spec=pltpu.PrefetchScalarGridSpec(
            num_scalar_prefetch=1,
            grid=(columns // block,),
            in_specs=[
                pl.BlockSpec((experts, 4, 256), lambda n, m: (0, 0, 0), pipeline_mode=once),
                pl.BlockSpec((experts, 4, 256), lambda n, m: (0, 0, 0), pipeline_mode=once),
                pl.BlockSpec((experts, 5 * STEP, ff), lambda n, m: (0, 0, 0), pipeline_mode=once),
                pl.BlockSpec((experts, ff, block), lambda n, m: (0, 0, n + start // block)),
            ],
            out_specs=[
                pl.BlockSpec((256, block), lambda n, m: (0, n)),
                pl.BlockSpec((256, block), lambda n, m: (0, n)),
                pl.BlockSpec((2, 256, block), lambda n, m: (0, 0, n)),
            ],
            scratch_shapes=[
                pltpu.VMEM((4, experts * STEP, 256), jnp.bfloat16),
                pltpu.VMEM((5 * STEP, block), jnp.bfloat16),
                pltpu.VMEM((4, experts * STEP, block), jnp.bfloat16),
            ],
        ),
        out_shape=[
            jax.ShapeDtypeStruct((256, columns), jnp.float32),
            jax.ShapeDtypeStruct((256, columns), jnp.float32),
            jax.ShapeDtypeStruct((2, 256, columns), jnp.bfloat16),
        ],
        compiler_params=pltpu.CompilerParams(
            vmem_limit_bytes=VMEM, dimension_semantics=("arbitrary",)
        ),
        cost_estimate=pl.CostEstimate(
            flops=experts * 300 * columns * ff * 2,
            bytes_accessed=experts * columns * ff * 2,
            transcendentals=0,
        ),
        name="down",
    )(meta, code, gate, h, w_down)


def layer(x, expert, slot, gate, w_gate, w_up, w_down, s_gate, s_up, s_down):
    local = w_gate.shape[0]
    experts = 4 * local
    x, expert, slot, gate = x[0, 0], expert[0, 0], slot[0, 0], gate[0, 0]
    tokens, top = expert.shape
    slots = 5 * tokens * top // (4 * experts)
    same = functools.partial(lax.ppermute, axis_name="ep", perm=SAME)
    cross = functools.partial(lax.ppermute, axis_name="ep", perm=CROSS)

    def everyone(v):
        far = cross(v)
        return [v, same(v), far, same(far)]

    table = tables(expert, slot, gate, experts, slots)
    table = jnp.stack(everyone(table))
    table = lax.dynamic_slice_in_dim(table, lax.axis_index("ep") * local, local, 2)
    code = table[:, 0].transpose(1, 0, 2).astype(jnp.int32)
    weight = table[:, 1].transpose(1, 0, 2)
    used = (jnp.max(code, -1) + 16) // 16 * 16
    ends = jnp.cumsum(used, 1)
    meta = jnp.concatenate([ends - used, ends[:, 3:], jnp.zeros((local, 3), jnp.int32)], 1)
    meta = meta.reshape(-1)

    x_first = everyone(x[:, :FIRST])
    x_rest = everyone(x[:, FIRST:])

    def dot(a, b):
        return jnp.dot(a, b, preferred_element_type=jnp.float32)

    hidden = (jax.nn.silu(dot(x, s_gate)) * dot(x, s_up)).astype(jnp.bfloat16)
    shared = dot(hidden, s_down)

    partial = up(meta, code, x_first, w_gate, w_up, 0, 1024)
    h = up(meta, code, x_rest, w_gate, w_up, FIRST, 512, partial)

    pieces, start = [], 0
    for columns in CHUNKS:
        own, far, near = down(meta, code, weight, h, w_down, start, columns, 512)
        near = same(near)
        far = cross((far + near[1].astype(jnp.float32)).astype(jnp.bfloat16))
        total = own + near[0].astype(jnp.float32) + far.astype(jnp.float32)
        total = total + shared[:, start : start + columns]
        pieces.append(total.astype(jnp.bfloat16))
        start += columns
    return jnp.concatenate(pieces, 1)[None, None]


def solution(mesh):
    rows, whole = P("dp", "ep"), P()
    return jax.shard_map(
        layer,
        mesh=mesh,
        in_specs=(rows,) * 4 + (P("ep"),) * 3 + (whole,) * 3,
        out_specs=rows,
        check_vma=False,
    )
```

```python
import functools

import jax
import jax.numpy as jnp
from jax import lax
from jax.experimental import pallas as pl
from jax.experimental.pallas import tpu as pltpu
from jax.sharding import PartitionSpec as P

SAME = [(0, 1), (1, 0), (2, 3), (3, 2)]
CROSS = [(0, 2), (1, 3), (2, 0), (3, 1)]
STEP = 112
EARLY = 2
CHUNKS = (1024, 3072, 3072)
VMEM = 63 * 2**20
KB = 1024
F32, BF16 = jnp.float32, jnp.bfloat16


def silu(g):
    return g / (1.0 + jnp.exp(-g))


def dot(a, b):
    return jnp.dot(a, b, preferred_element_type=F32)


def tables(expert, slot, gate, experts, slots):
    expert, slot, gate = expert.T, slot.T, gate.T
    hit = (expert[None] == jnp.arange(experts)[:, None, None]) & (slot < slots)[None]
    code = jnp.sum(jnp.where(hit, slot[None] + 1, 0), 1) - 1
    weight = jnp.sum(jnp.where(hit, gate[None], 0.0), 1)
    return jnp.stack([code.astype(F32), weight])


def arrive_kernel(
    local, x, table, w_gate, w_up, s_gate, s_up, s_down,
    xs, tabs, h, shared,
    got, tab, ring, ring2, acc_s, acc, z, hidden, stage,
    ring_sem, ring2_sem, stage_sem, cross_send, cross_recv, pass_send, pass_recv,
    own_send, own_recv, tab_send, tab_recv, out_sem,
):
    d, ff = x.shape[1], s_gate.shape[1]
    chunks = d // KB
    me = lax.axis_index("ep")
    partner, across = me + 1 - 2 * lax.rem(me, 2), lax.rem(me + 2, 4)
    peers = (partner, across, 3 - me)

    barrier = pltpu.get_barrier_semaphore()
    for peer in peers:
        pl.semaphore_signal(
            barrier, inc=1, device_id={"ep": peer}, device_id_type=pl.DeviceIdType.MESH
        )
    pl.semaphore_wait(barrier, 3)

    def remote(src, dst, send, recv, peer):
        return pltpu.make_async_remote_copy(
            src, dst, send, recv, device_id={"ep": peer}, device_id_type=pl.DeviceIdType.MESH
        )

    def columns(k):
        return pl.ds(pl.multiple_of(k * KB, KB), KB)

    def cross(k):
        c = columns(k)
        return remote(x.at[:, c], got.at[1, :, c], cross_send.at[k], cross_recv.at[k], across)

    def onward(k):
        c = columns(k)
        return remote(
            got.at[1, :, c], got.at[2, :, c], pass_send.at[k], pass_recv.at[k], partner
        )

    own = remote(x, got.at[0], own_send, own_recv, partner)
    tab_copies = [
        remote(table, tab.at[i], tab_send.at[i], tab_recv.at[i], peer)
        for i, peer in enumerate(peers)
    ]

    def keep(i, k):
        c = columns(k)
        return pltpu.make_async_copy(got.at[i, :, c], xs.at[i, :, c], out_sem.at[i, k])

    n_shared = 2 * chunks
    n_all = n_shared + 2 * EARLY * chunks
    slots = ring.shape[0]

    def fetch(j):
        slot = lax.rem(j, slots)

        def go(src):
            pltpu.make_async_copy(src, ring.at[slot], ring_sem.at[slot]).start()

        for i, w in enumerate((s_gate, s_up)):

            @pl.when((j < n_shared) & (lax.rem(j, 2) == i))
            def _(w=w):
                go(w.at[columns(j // 2), :])

        i = jnp.maximum(j - n_shared, 0)
        k, q = i // (2 * EARLY), lax.rem(i, 2 * EARLY)
        for s, w in enumerate((w_gate, w_up)):

            @pl.when((j >= n_shared) & (j < n_all) & (lax.rem(q, 2) == s))
            def _(w=w):
                go(w.at[q // 2, columns(k), :])

    def ready(j):
        slot = lax.rem(j, slots)
        pltpu.make_async_copy(s_gate.at[:KB, :], ring.at[slot], ring_sem.at[slot]).wait()
        return slot

    wide = ring2.shape[2]

    def down_tile(n):
        slot = lax.rem(n, 2)
        c = pl.ds(pl.multiple_of(n * wide, wide), wide)
        return pltpu.make_async_copy(s_down.at[:, c], ring2.at[slot], ring2_sem.at[slot])

    def put(n):
        slot = lax.rem(n, 2)
        c = pl.ds(pl.multiple_of(n * wide, wide), wide)
        return pltpu.make_async_copy(stage.at[slot], shared.at[:, c], stage_sem.at[slot])

    for copy in tab_copies:
        copy.start()

    @pl.loop(0, chunks)
    def _(k):
        cross(k).start()

    own.start()
    for j in range(slots):
        fetch(jnp.int32(j))
    down_tile(0).start()
    down_tile(1).start()

    acc_s[...] = jnp.zeros_like(acc_s)

    @pl.loop(0, n_shared)
    def _(j):
        slot = ready(j)
        a = x[:, columns(j // 2)]
        side = lax.rem(j, 2)
        for n in range(ff // 512):
            c = slice(n * 512, n * 512 + 512)
            acc_s[side, :, c] += dot(a, ring[slot, :, c])
        fetch(j + slots)

    for n in range(ff // 512):
        c = slice(n * 512, n * 512 + 512)
        hidden[:, c] = (silu(acc_s[0, :, c]) * acc_s[1, :, c]).astype(BF16)

    n_down = d // wide

    @pl.loop(0, n_down)
    def _(n):
        down_tile(n).wait()

        @pl.when(n >= 2)
        def _():
            put(n - 2).wait()

        slot = lax.rem(n, 2)
        stage[slot] = dot(hidden[...], ring2[slot])

        @pl.when(n + 2 < n_down)
        def _():
            down_tile(n + 2).start()

        put(n).start()

    put(n_down - 2).wait()
    put(n_down - 1).wait()

    for copy in tab_copies:
        copy.wait()
    tabs[0] = table[...]
    for i in range(3):
        tabs[1 + i] = tab[i]
    own.wait()

    acc[...] = jnp.zeros_like(acc)
    rows = lax.broadcasted_iota(jnp.int32, (STEP, 256), 0).astype(F32)

    @pl.loop(0, chunks)
    def _(k):
        c = columns(k)
        cross(k).wait_recv()
        onward(k).start()
        keep(0, k).start()
        keep(1, k).start()

        def picked(i, a):
            parts = []
            for e in range(EARLY):
                t = table if i == 0 else tab.at[i - 1]
                code = t[0, pl.ds(me * local + e, 1), :]
                parts.append((rows == code).astype(BF16))
            z_i = dot(jnp.concatenate(parts, 0), a).astype(BF16)
            for e in range(EARLY):
                z[e, i * STEP : (i + 1) * STEP, :] = z_i[e * STEP : (e + 1) * STEP, :]

        picked(0, x[:, c])
        picked(1, got[0, :, c])
        picked(2, got[1, :, c])
        onward(k).wait_recv()
        keep(2, k).start()
        picked(3, got[2, :, c])

        @pl.loop(0, 2 * EARLY)
        def _(q):
            j = n_shared + 2 * EARLY * k + q
            slot = ready(j)
            for n in range(ff // 512):
                cc = slice(n * 512, n * 512 + 512)
                acc[q, :, cc] += dot(z[q // 2], ring[slot, :, cc])
            fetch(j + slots)

    for e in range(EARLY):
        for n in range(ff // 512):
            c = slice(n * 512, n * 512 + 512)
            g, u = acc[2 * e, :, c], acc[2 * e + 1, :, c]
            h[e, :, c] = (silu(g) * u).astype(BF16)

    @pl.loop(0, chunks)
    def _(k):
        cross(k).wait_send()
        onward(k).wait_send()
        for i in range(3):
            keep(i, k).wait()


def arrive(x, table, w_gate, w_up, s_gate, s_up, s_down):
    tokens, d = x.shape
    local, _, ff = w_gate.shape
    chunks = d // KB
    vmem, hbm = pl.BlockSpec(memory_space=pltpu.VMEM), pl.BlockSpec(memory_space=pl.ANY)
    dma = pltpu.SemaphoreType.DMA
    return pl.pallas_call(
        functools.partial(arrive_kernel, local),
        in_specs=[vmem] * 2 + [hbm] * 5,
        out_specs=[hbm, vmem, vmem, hbm],
        out_shape=[
            jax.ShapeDtypeStruct((3, tokens, d), BF16),
            jax.ShapeDtypeStruct((4, *table.shape), F32),
            jax.ShapeDtypeStruct((EARLY, 4 * STEP, ff), BF16),
            jax.ShapeDtypeStruct((tokens, d), F32),
        ],
        scratch_shapes=[
            pltpu.VMEM((3, tokens, d), BF16),
            pltpu.VMEM((3, *table.shape), F32),
            pltpu.VMEM((3, KB, ff), BF16),
            pltpu.VMEM((2, ff, 512), BF16),
            pltpu.VMEM((2, tokens, ff), F32),
            pltpu.VMEM((2 * EARLY, 4 * STEP, ff), F32),
            pltpu.VMEM((EARLY, 4 * STEP, KB), BF16),
            pltpu.VMEM((tokens, ff), BF16),
            pltpu.VMEM((2, tokens, 512), F32),
            dma((3,)), dma((2,)), dma((2,)),
            dma((chunks,)), dma((chunks,)), dma((chunks,)), dma((chunks,)),
            dma, dma, dma((3,)), dma((3,)), dma((3, chunks)),
        ],
        compiler_params=pltpu.CompilerParams(
            collective_id=0, has_side_effects=True, vmem_limit_bytes=VMEM
        ),
        name="arrive",
    )(x, table, w_gate, w_up, s_gate, s_up, s_down)


def up_kernel(block, meta, code, x0, x1, wg, wu, h_out, z):
    depth = x0.shape[1]
    e, n = pl.program_id(0), pl.program_id(1)
    at_meta = (e + EARLY) * 8
    total = pl.multiple_of(meta[at_meta + 4], 16)

    @pl.when(n == 0)
    def _():
        rows = lax.broadcasted_iota(jnp.int32, (STEP, 256), 0)
        picks = [(rows == code[0, k : k + 1, :]).astype(BF16) for k in range(4)]

        @pl.loop(0, depth // 1024)
        def _(c):
            cols = pl.ds(pl.multiple_of(c * 1024, 1024), 1024)
            parts = [
                dot(picks[k], x0[:, cols] if k == 0 else x1[k - 1, :, cols]).astype(BF16)
                for k in range(4)
            ]
            for k in range(4):
                at = pl.multiple_of(meta[at_meta + k], 16)
                z[pl.ds(at, STEP), cols] = parts[k]

        z[pl.ds(total, STEP), :] = jnp.zeros((STEP, depth), BF16)

    size = (total + STEP - 1) // STEP
    for v in range(1, 5):

        @pl.when(size == v)
        def _(v=v):
            m = v * STEP
            g = dot(z[:m, :], wg[0])
            u = dot(z[:m, :], wu[0])
            h_out[0, :m, :] = (silu(g) * u).astype(BF16)


def up(meta, code, x0, x1, w_gate, w_up, block):
    experts, depth, ff = w_gate.shape
    late = experts - EARLY
    once = pl.Buffered(1)
    weight = pl.BlockSpec((1, depth, block), lambda e, n, m: (e + EARLY, 0, n))
    return pl.pallas_call(
        functools.partial(up_kernel, block),
        grid_spec=pltpu.PrefetchScalarGridSpec(
            num_scalar_prefetch=1,
            grid=(late, ff // block),
            in_specs=[
                pl.BlockSpec((1, 4, 256), lambda e, n, m: (e + EARLY, 0, 0)),
                pl.BlockSpec((256, depth), lambda e, n, m: (0, 0), pipeline_mode=once),
                pl.BlockSpec((3, 256, depth), lambda e, n, m: (0, 0, 0), pipeline_mode=once),
                weight,
                weight,
            ],
            out_specs=pl.BlockSpec((1, 4 * STEP, block), lambda e, n, m: (e, 0, n)),
            scratch_shapes=[pltpu.VMEM((5 * STEP, depth), BF16)],
        ),
        out_shape=jax.ShapeDtypeStruct((late, 4 * STEP, ff), BF16),
        compiler_params=pltpu.CompilerParams(
            vmem_limit_bytes=VMEM, dimension_semantics=("arbitrary", "arbitrary")
        ),
        cost_estimate=pl.CostEstimate(
            flops=late * 300 * depth * ff * 4,
            bytes_accessed=late * depth * ff * 4,
            transcendentals=0,
        ),
        name="up",
    )(meta, code, x0, x1, w_gate, w_up)


def down_kernel(experts, meta, code, gate, early, late, wd, own, far, near, h, wt, tmp, stack, sem):
    first = pl.program_id(0) == 0

    def load(e):
        if e < EARLY:
            return pltpu.make_async_copy(early.at[e], h.at[e], sem.at[e])
        return pltpu.make_async_copy(late.at[e - EARLY], h.at[e], sem.at[e])

    @pl.when(first)
    def _():
        for e in range(experts):
            load(e).start()
        tmp[...] = jnp.zeros_like(tmp)
        stack[...] = jnp.zeros_like(stack)
        rows = lax.broadcasted_iota(jnp.int32, (STEP, 256), 0)
        for k in range(4):
            parts = [
                jnp.where(rows == code[e, k : k + 1, :], gate[e, k : k + 1, :], 0.0)
                for e in range(experts)
            ]
            parts.append(jnp.zeros((stack.shape[1] - experts * STEP, 256), F32))
            wt[k] = jnp.concatenate(parts, 0).T.astype(BF16)
        for e in range(experts):
            load(e).wait()

    @pl.loop(0, experts)
    def _(e):
        total = meta[e * 8 + 4]
        size = (total + STEP - 1) // STEP
        for v in range(1, 5):

            @pl.when(size == v)
            def _(v=v):
                m = v * STEP
                tmp[:m, :] = dot(h[e, :m, :], wd[e]).astype(BF16)

        to = pl.ds(pl.multiple_of(e * STEP, STEP), STEP)
        for k in range(4):
            at = pl.multiple_of(meta[e * 8 + k], 16)
            stack[k, to, :] = tmp[pl.ds(at, STEP), :]

    near[0] = dot(wt[1], stack[1]).astype(BF16)
    near[1] = dot(wt[3], stack[3]).astype(BF16)
    far[...] = dot(wt[2], stack[2])
    own[...] = dot(wt[0], stack[0])


def down(meta, code, gate, early, late, w_down, start, columns, block):
    experts, ff, _ = w_down.shape
    once = pl.Buffered(1)
    small = pl.BlockSpec((experts, 4, 256), lambda n, m: (0, 0, 0), pipeline_mode=once)
    depth = -(-experts * STEP // 256) * 256
    return pl.pallas_call(
        functools.partial(down_kernel, experts),
        grid_spec=pltpu.PrefetchScalarGridSpec(
            num_scalar_prefetch=1,
            grid=(columns // block,),
            in_specs=[
                small,
                small,
                pl.BlockSpec(memory_space=pl.ANY),
                pl.BlockSpec(memory_space=pl.ANY),
                pl.BlockSpec((experts, ff, block), lambda n, m: (0, 0, n + start // block)),
            ],
            out_specs=[
                pl.BlockSpec((256, block), lambda n, m: (0, n)),
                pl.BlockSpec((256, block), lambda n, m: (0, n)),
                pl.BlockSpec((2, 256, block), lambda n, m: (0, 0, n)),
            ],
            scratch_shapes=[
                pltpu.VMEM((experts, 4 * STEP, ff), BF16),
                pltpu.VMEM((4, 256, depth), BF16),
                pltpu.VMEM((5 * STEP, block), BF16),
                pltpu.VMEM((4, depth, block), BF16),
                pltpu.SemaphoreType.DMA((experts,)),
            ],
        ),
        out_shape=[
            jax.ShapeDtypeStruct((256, columns), F32),
            jax.ShapeDtypeStruct((256, columns), F32),
            jax.ShapeDtypeStruct((2, 256, columns), BF16),
        ],
        compiler_params=pltpu.CompilerParams(
            vmem_limit_bytes=VMEM, dimension_semantics=("arbitrary",)
        ),
        cost_estimate=pl.CostEstimate(
            flops=experts * 300 * columns * ff * 2,
            bytes_accessed=experts * columns * ff * 2,
            transcendentals=0,
        ),
        name="down",
    )(meta, code, gate, early, late, w_down)


def layer(x, expert, slot, gate, w_gate, w_up, w_down, s_gate, s_up, s_down):
    local = w_gate.shape[0]
    experts = 4 * local
    x, expert, slot, gate = x[0, 0], expert[0, 0], slot[0, 0], gate[0, 0]
    tokens, top = expert.shape
    slots = 5 * tokens * top // (4 * experts)
    same = functools.partial(lax.ppermute, axis_name="ep", perm=SAME)
    cross = functools.partial(lax.ppermute, axis_name="ep", perm=CROSS)

    table = tables(expert, slot, gate, experts, slots)
    xs, table, early, shared = arrive(x, table, w_gate, w_up, s_gate, s_up, s_down)
    table = lax.dynamic_slice_in_dim(table, lax.axis_index("ep") * local, local, 2)
    code = table[:, 0].transpose(1, 0, 2).astype(jnp.int32)
    weight = table[:, 1].transpose(1, 0, 2)
    used = (jnp.max(code, -1) + 16) // 16 * 16
    used = jnp.where(jnp.arange(local)[:, None] < EARLY, STEP, used)
    starts = [jnp.zeros_like(used[:, 0])]
    for k in range(4):
        starts.append(starts[-1] + used[:, k])
    meta = jnp.stack(starts + starts[:3], 1).reshape(-1)

    late = up(meta, code, x, xs, w_gate, w_up, 512)

    pieces, start = [], 0
    for columns in CHUNKS:
        own, far, near = down(meta, code, weight, early, late, w_down, start, columns, 512)
        meta, own = lax.optimization_barrier((meta, own))
        near = same(near)
        far = cross((far + near[1].astype(F32)).astype(BF16))
        total = own + near[0].astype(F32) + far.astype(F32)
        total = total + shared[:, start : start + columns]
        pieces.append(total.astype(BF16))
        start += columns
    return jnp.concatenate(pieces, 1)[None, None]


def solution(mesh):
    rows, whole = P("dp", "ep"), P()
    return jax.shard_map(
        layer,
        mesh=mesh,
        in_specs=(rows,) * 4 + (P("ep"),) * 3 + (whole,) * 3,
        out_specs=rows,
        check_vma=False,
    )
```

```python
import functools

import jax
import jax.numpy as jnp
from jax import lax
from jax.experimental import pallas as pl
from jax.experimental.pallas import tpu as pltpu
from jax.sharding import PartitionSpec as P

STEP = 112
EARLY = 2
VMEM = 63 * 2**20
KB = 1024
F32, BF16 = jnp.float32, jnp.bfloat16


def silu(g):
    return g / (1.0 + jnp.exp(-g))


def dot(a, b):
    return jnp.dot(a, b, preferred_element_type=F32)


def tables(expert, slot, gate, experts, slots):
    expert, slot, gate = expert.T, slot.T, gate.T
    hit = (expert[None] == jnp.arange(experts)[:, None, None]) & (slot < slots)[None]
    code = jnp.sum(jnp.where(hit, slot[None] + 1, 0), 1) - 1
    weight = jnp.sum(jnp.where(hit, gate[None], 0.0), 1)
    return jnp.stack([code.astype(F32), weight])


def arrive_kernel(
    local, x, table, w_gate, w_up, s_gate, s_up, s_down,
    xs, tabs, h, shared,
    got, tab, ring, ring2, acc_s, acc, z, hidden, stage,
    ring_sem, ring2_sem, stage_sem, cross_send, cross_recv, pass_send, pass_recv,
    own_send, own_recv, tab_send, tab_recv, out_sem,
):
    d, ff = x.shape[1], s_gate.shape[1]
    chunks = d // KB
    me = lax.axis_index("ep")
    partner, across = me + 1 - 2 * lax.rem(me, 2), lax.rem(me + 2, 4)
    peers = (partner, across, 3 - me)

    barrier = pltpu.get_barrier_semaphore()
    for peer in peers:
        pl.semaphore_signal(
            barrier, inc=1, device_id={"ep": peer}, device_id_type=pl.DeviceIdType.MESH
        )
    pl.semaphore_wait(barrier, 3)

    def remote(src, dst, send, recv, peer):
        return pltpu.make_async_remote_copy(
            src, dst, send, recv, device_id={"ep": peer}, device_id_type=pl.DeviceIdType.MESH
        )

    def columns(k):
        return pl.ds(pl.multiple_of(k * KB, KB), KB)

    def cross(k):
        c = columns(k)
        return remote(x.at[:, c], got.at[1, :, c], cross_send.at[k], cross_recv.at[k], across)

    def onward(k):
        c = columns(k)
        return remote(
            got.at[1, :, c], got.at[2, :, c], pass_send.at[k], pass_recv.at[k], partner
        )

    own = remote(x, got.at[0], own_send, own_recv, partner)
    tab_copies = [
        remote(table, tab.at[i], tab_send.at[i], tab_recv.at[i], peer)
        for i, peer in enumerate(peers)
    ]

    def keep(i, k):
        c = columns(k)
        return pltpu.make_async_copy(got.at[i, :, c], xs.at[i, :, c], out_sem.at[i, k])

    n_shared = 2 * chunks
    n_all = n_shared + 2 * EARLY * chunks
    slots = ring.shape[0]

    def fetch(j):
        slot = lax.rem(j, slots)

        def go(src):
            pltpu.make_async_copy(src, ring.at[slot], ring_sem.at[slot]).start()

        for i, w in enumerate((s_gate, s_up)):

            @pl.when((j < n_shared) & (lax.rem(j, 2) == i))
            def _(w=w):
                go(w.at[columns(j // 2), :])

        i = jnp.maximum(j - n_shared, 0)
        k, q = i // (2 * EARLY), lax.rem(i, 2 * EARLY)
        for s, w in enumerate((w_gate, w_up)):

            @pl.when((j >= n_shared) & (j < n_all) & (lax.rem(q, 2) == s))
            def _(w=w):
                go(w.at[q // 2, columns(k), :])

    def ready(j):
        slot = lax.rem(j, slots)
        pltpu.make_async_copy(s_gate.at[:KB, :], ring.at[slot], ring_sem.at[slot]).wait()
        return slot

    wide = ring2.shape[2]

    def down_tile(n):
        slot = lax.rem(n, 2)
        c = pl.ds(pl.multiple_of(n * wide, wide), wide)
        return pltpu.make_async_copy(s_down.at[:, c], ring2.at[slot], ring2_sem.at[slot])

    def put(n):
        slot = lax.rem(n, 2)
        c = pl.ds(pl.multiple_of(n * wide, wide), wide)
        return pltpu.make_async_copy(stage.at[slot], shared.at[:, c], stage_sem.at[slot])

    for copy in tab_copies:
        copy.start()

    @pl.loop(0, chunks)
    def _(k):
        cross(k).start()

    own.start()
    for j in range(slots):
        fetch(jnp.int32(j))
    down_tile(0).start()
    down_tile(1).start()

    acc_s[...] = jnp.zeros_like(acc_s)

    @pl.loop(0, n_shared)
    def _(j):
        slot = ready(j)
        a = x[:, columns(j // 2)]
        side = lax.rem(j, 2)
        for n in range(ff // 512):
            c = slice(n * 512, n * 512 + 512)
            acc_s[side, :, c] += dot(a, ring[slot, :, c])
        fetch(j + slots)

    for n in range(ff // 512):
        c = slice(n * 512, n * 512 + 512)
        hidden[:, c] = (silu(acc_s[0, :, c]) * acc_s[1, :, c]).astype(BF16)

    n_down = d // wide

    @pl.loop(0, n_down)
    def _(n):
        down_tile(n).wait()

        @pl.when(n >= 2)
        def _():
            put(n - 2).wait()

        slot = lax.rem(n, 2)
        stage[slot] = dot(hidden[...], ring2[slot])

        @pl.when(n + 2 < n_down)
        def _():
            down_tile(n + 2).start()

        put(n).start()

    put(n_down - 2).wait()
    put(n_down - 1).wait()

    for copy in tab_copies:
        copy.wait()
    tabs[0] = table[...]
    for i in range(3):
        tabs[1 + i] = tab[i]
    own.wait()

    acc[...] = jnp.zeros_like(acc)
    rows = lax.broadcasted_iota(jnp.int32, (STEP, 256), 0).astype(F32)

    @pl.loop(0, chunks)
    def _(k):
        c = columns(k)
        cross(k).wait_recv()
        onward(k).start()
        keep(0, k).start()
        keep(1, k).start()

        def picked(i, a):
            parts = []
            for e in range(EARLY):
                t = table if i == 0 else tab.at[i - 1]
                code = t[0, pl.ds(me * local + e, 1), :]
                parts.append((rows == code).astype(BF16))
            z_i = dot(jnp.concatenate(parts, 0), a).astype(BF16)
            for e in range(EARLY):
                z[e, i * STEP : (i + 1) * STEP, :] = z_i[e * STEP : (e + 1) * STEP, :]

        picked(0, x[:, c])
        picked(1, got[0, :, c])
        picked(2, got[1, :, c])
        onward(k).wait_recv()
        keep(2, k).start()
        picked(3, got[2, :, c])

        @pl.loop(0, 2 * EARLY)
        def _(q):
            j = n_shared + 2 * EARLY * k + q
            slot = ready(j)
            for n in range(ff // 512):
                cc = slice(n * 512, n * 512 + 512)
                acc[q, :, cc] += dot(z[q // 2], ring[slot, :, cc])
            fetch(j + slots)

    for e in range(EARLY):
        for n in range(ff // 512):
            c = slice(n * 512, n * 512 + 512)
            g, u = acc[2 * e, :, c], acc[2 * e + 1, :, c]
            h[e, :, c] = (silu(g) * u).astype(BF16)

    @pl.loop(0, chunks)
    def _(k):
        cross(k).wait_send()
        onward(k).wait_send()
        for i in range(3):
            keep(i, k).wait()


def arrive(x, table, w_gate, w_up, s_gate, s_up, s_down):
    tokens, d = x.shape
    local, _, ff = w_gate.shape
    chunks = d // KB
    vmem, hbm = pl.BlockSpec(memory_space=pltpu.VMEM), pl.BlockSpec(memory_space=pl.ANY)
    dma = pltpu.SemaphoreType.DMA
    return pl.pallas_call(
        functools.partial(arrive_kernel, local),
        in_specs=[vmem] * 2 + [hbm] * 5,
        out_specs=[hbm, vmem, vmem, hbm],
        out_shape=[
            jax.ShapeDtypeStruct((3, tokens, d), BF16),
            jax.ShapeDtypeStruct((4, *table.shape), F32),
            jax.ShapeDtypeStruct((EARLY, 4 * STEP, ff), BF16),
            jax.ShapeDtypeStruct((tokens, d), F32),
        ],
        scratch_shapes=[
            pltpu.VMEM((3, tokens, d), BF16),
            pltpu.VMEM((3, *table.shape), F32),
            pltpu.VMEM((3, KB, ff), BF16),
            pltpu.VMEM((2, ff, 512), BF16),
            pltpu.VMEM((2, tokens, ff), F32),
            pltpu.VMEM((2 * EARLY, 4 * STEP, ff), F32),
            pltpu.VMEM((EARLY, 4 * STEP, KB), BF16),
            pltpu.VMEM((tokens, ff), BF16),
            pltpu.VMEM((2, tokens, 512), F32),
            dma((3,)), dma((2,)), dma((2,)),
            dma((chunks,)), dma((chunks,)), dma((chunks,)), dma((chunks,)),
            dma, dma, dma((3,)), dma((3,)), dma((3, chunks)),
        ],
        compiler_params=pltpu.CompilerParams(
            collective_id=0, has_side_effects=True, vmem_limit_bytes=VMEM
        ),
        name="arrive",
    )(x, table, w_gate, w_up, s_gate, s_up, s_down)


def up_kernel(block, meta, code, x0, x1, wg, wu, h_out, z, packed):
    depth = x0.shape[1]
    e, n = pl.program_id(0), pl.program_id(1)
    at_meta = (e + EARLY) * 8
    total = pl.multiple_of(meta[at_meta + 4], 16)

    @pl.when(n == 0)
    def _():
        rows = lax.broadcasted_iota(jnp.int32, (STEP, 256), 0)
        picks = [(rows == code[0, k : k + 1, :]).astype(BF16) for k in range(4)]

        @pl.loop(0, depth // 1024)
        def _(c):
            cols = pl.ds(pl.multiple_of(c * 1024, 1024), 1024)
            parts = [
                dot(picks[k], x0[:, cols] if k == 0 else x1[k - 1, :, cols]).astype(BF16)
                for k in range(4)
            ]
            for k in range(4):
                at = pl.multiple_of(meta[at_meta + k], 16)
                z[pl.ds(at, STEP), cols] = parts[k]

        z[pl.ds(total, STEP), :] = jnp.zeros((STEP, depth), BF16)

    size = (total + STEP - 1) // STEP
    @pl.when(size == 0)
    def _():
        h_out[...] = jnp.zeros_like(h_out)

    for v in range(1, 5):

        @pl.when(size == v)
        def _(v=v):
            m = v * STEP
            g = dot(z[:m, :], wg[0])
            u = dot(z[:m, :], wu[0])
            packed[:m, :] = (silu(g) * u).astype(BF16)
            packed[m : m + STEP, :] = jnp.zeros((STEP, block), BF16)
            for k in range(4):
                at = pl.multiple_of(meta[at_meta + k], 16)
                h_out[0, k * STEP : (k + 1) * STEP, :] = packed[pl.ds(at, STEP), :]


def up(meta, code, x0, x1, w_gate, w_up, block):
    experts, depth, ff = w_gate.shape
    late = experts - EARLY
    once = pl.Buffered(1)
    weight = pl.BlockSpec((1, depth, block), lambda e, n, m: (e + EARLY, 0, n))
    return pl.pallas_call(
        functools.partial(up_kernel, block),
        grid_spec=pltpu.PrefetchScalarGridSpec(
            num_scalar_prefetch=1,
            grid=(late, ff // block),
            in_specs=[
                pl.BlockSpec((1, 4, 256), lambda e, n, m: (e + EARLY, 0, 0)),
                pl.BlockSpec((256, depth), lambda e, n, m: (0, 0), pipeline_mode=once),
                pl.BlockSpec((3, 256, depth), lambda e, n, m: (0, 0, 0), pipeline_mode=once),
                weight,
                weight,
            ],
            out_specs=pl.BlockSpec((1, 4 * STEP, block), lambda e, n, m: (e, 0, n)),
            scratch_shapes=[
                pltpu.VMEM((5 * STEP, depth), BF16),
                pltpu.VMEM((5 * STEP, block), BF16),
            ],
        ),
        out_shape=jax.ShapeDtypeStruct((late, 4 * STEP, ff), BF16),
        compiler_params=pltpu.CompilerParams(
            vmem_limit_bytes=VMEM, dimension_semantics=("arbitrary", "arbitrary")
        ),
        cost_estimate=pl.CostEstimate(
            flops=late * 300 * depth * ff * 4,
            bytes_accessed=late * depth * ff * 4,
            transcendentals=0,
        ),
        name="up",
    )(meta, code, x0, x1, w_gate, w_up)


def finish_kernel(
    chunks, code, gate, early, late, wd, shared, y,
    h, wt, stack, own, far, near, near_got, out, out_got,
    sem, near_send, near_recv, out_send, out_recv,
):
    experts, block = wd.shape[0], wd.shape[2]
    i = pl.program_id(0)
    me = lax.axis_index("ep")
    partner, across = me + 1 - 2 * lax.rem(me, 2), lax.rem(me + 2, 4)

    def remote(src, dst, send, recv, peer):
        return pltpu.make_async_remote_copy(
            src, dst, send, recv, device_id={"ep": peer}, device_id_type=pl.DeviceIdType.MESH
        )

    def to_partner(j):
        return remote(
            near.at[lax.rem(j, 2)], near_got.at[j], near_send.at[lax.rem(j, 2)], near_recv.at[j],
            partner,
        )

    def to_across(j):
        return remote(
            out.at[lax.rem(j, 2)], out_got.at[j], out_send.at[lax.rem(j, 2)], out_recv.at[j],
            across,
        )

    def load(e):
        src = early.at[e] if e < EARLY else late.at[e - EARLY]
        return pltpu.make_async_copy(src, h.at[e], sem.at[e])

    @pl.when(i == 0)
    def _():
        barrier = pltpu.get_barrier_semaphore()
        for peer in (partner, across):
            pl.semaphore_signal(
                barrier, inc=1, device_id={"ep": peer}, device_id_type=pl.DeviceIdType.MESH
            )
        for e in range(experts):
            load(e).start()
        stack[...] = jnp.zeros_like(stack)
        rows = lax.broadcasted_iota(jnp.int32, (STEP, 256), 0)
        for k in range(4):
            parts = [
                jnp.where(rows == code[e, k : k + 1, :], gate[e, k : k + 1, :], 0.0)
                for e in range(experts)
            ]
            parts.append(jnp.zeros((stack.shape[1] - experts * STEP, 256), F32))
            wt[k] = jnp.concatenate(parts, 0).T.astype(BF16)
        for e in range(experts):
            load(e).wait()
        pl.semaphore_wait(barrier, 2)

    @pl.when((i >= 1) & (i <= chunks))
    def _():
        j = i - 1

        @pl.when(j >= 2)
        def _():
            to_across(j - 2).wait_send()

        to_partner(j).wait_recv()
        out[lax.rem(j, 2)] = (far[...] + near_got[j, 1].astype(F32)).astype(BF16)

    @pl.when(i >= 2)
    def _():
        j = i - 2
        to_across(j).wait_recv()
        total = own[lax.rem(j, 3)] + near_got[j, 0].astype(F32) + out_got[j].astype(F32)
        y[...] = (total + shared[...]).astype(BF16)

    @pl.when((i >= 1) & (i <= chunks))
    def _():
        to_across(i - 1).start()

    @pl.when(i < chunks)
    def _():
        for e in range(experts):
            made = dot(h[e], wd[e]).astype(BF16)
            for k in range(4):
                stack[k, e * STEP : (e + 1) * STEP, :] = made[k * STEP : (k + 1) * STEP, :]

        @pl.when(i >= 2)
        def _():
            to_partner(i - 2).wait_send()

        slot = lax.rem(i, 2)
        near[slot, 1] = dot(wt[3], stack[3]).astype(BF16)
        near[slot, 0] = dot(wt[1], stack[1]).astype(BF16)
        far[...] = dot(wt[2], stack[2])
        to_partner(i).start()
        own[lax.rem(i, 3)] = dot(wt[0], stack[0])

    @pl.when(i == chunks + 1)
    def _():
        for j in (chunks - 2, chunks - 1):
            to_partner(j).wait_send()
            to_across(j).wait_send()


def finish(code, gate, early, late, w_down, shared, block):
    experts, ff, d = w_down.shape
    chunks = d // block
    once = pl.Buffered(1)
    small = pl.BlockSpec((experts, 4, 256), lambda i: (0, 0, 0), pipeline_mode=once)
    result = pl.BlockSpec((256, block), lambda i: (0, jnp.maximum(i - 2, 0)))
    depth = -(-experts * STEP // 256) * 256
    dma = pltpu.SemaphoreType.DMA
    return pl.pallas_call(
        functools.partial(finish_kernel, chunks),
        grid=(chunks + 2,),
        in_specs=[
            small,
            small,
            pl.BlockSpec(memory_space=pl.ANY),
            pl.BlockSpec(memory_space=pl.ANY),
            pl.BlockSpec((experts, ff, block), lambda i: (0, 0, jnp.minimum(i, chunks - 1))),
            result,
        ],
        out_specs=result,
        scratch_shapes=[
            pltpu.VMEM((experts, 4 * STEP, ff), BF16),
            pltpu.VMEM((4, 256, depth), BF16),
            pltpu.VMEM((4, depth, block), BF16),
            pltpu.VMEM((3, 256, block), F32),
            pltpu.VMEM((256, block), F32),
            pltpu.VMEM((2, 2, 256, block), BF16),
            pltpu.VMEM((chunks, 2, 256, block), BF16),
            pltpu.VMEM((2, 256, block), BF16),
            pltpu.VMEM((chunks, 256, block), BF16),
            dma((experts,)),
            dma((2,)),
            dma((chunks,)),
            dma((2,)),
            dma((chunks,)),
        ],
        out_shape=jax.ShapeDtypeStruct((256, d), BF16),
        compiler_params=pltpu.CompilerParams(
            collective_id=1,
            has_side_effects=True,
            vmem_limit_bytes=VMEM,
            dimension_semantics=("arbitrary",),
        ),
        name="finish",
    )(code, gate, early, late, w_down, shared)


def layer(x, expert, slot, gate, w_gate, w_up, w_down, s_gate, s_up, s_down):
    local = w_gate.shape[0]
    experts = 4 * local
    x, expert, slot, gate = x[0, 0], expert[0, 0], slot[0, 0], gate[0, 0]
    tokens, top = expert.shape
    slots = 5 * tokens * top // (4 * experts)
    table = tables(expert, slot, gate, experts, slots)
    xs, table, early, shared = arrive(x, table, w_gate, w_up, s_gate, s_up, s_down)
    table = lax.dynamic_slice_in_dim(table, lax.axis_index("ep") * local, local, 2)
    code = table[:, 0].transpose(1, 0, 2).astype(jnp.int32)
    weight = table[:, 1].transpose(1, 0, 2)
    used = (jnp.max(code, -1) + 16) // 16 * 16
    starts = [jnp.zeros_like(used[:, 0])]
    for k in range(4):
        starts.append(starts[-1] + used[:, k])
    meta = jnp.stack(starts + starts[:3], 1).reshape(-1)

    late = up(meta, code, x, xs, w_gate, w_up, 512)
    return finish(code, weight, early, late, w_down, shared, 512)[None, None]


def solution(mesh):
    rows, whole = P("dp", "ep"), P()
    return jax.shard_map(
        layer,
        mesh=mesh,
        in_specs=(rows,) * 4 + (P("ep"),) * 3 + (whole,) * 3,
        out_specs=rows,
        check_vma=False,
    )
```

```python
import functools

import jax
import jax.numpy as jnp
from jax import lax
from jax.experimental import pallas as pl
from jax.experimental.pallas import tpu as pltpu
from jax.sharding import PartitionSpec as P

STEP = 112
EARLY = 2
VMEM = 63 * 2**20
KB = 1024
F32, BF16 = jnp.float32, jnp.bfloat16


def silu(g):
    return g / (1.0 + jnp.exp(-g))


def dot(a, b):
    return jnp.dot(a, b, preferred_element_type=F32)


def tables(expert, slot, gate, experts, slots):
    expert, slot, gate = expert.T, slot.T, gate.T
    hit = (expert[None] == jnp.arange(experts)[:, None, None]) & (slot < slots)[None]
    code = jnp.sum(jnp.where(hit, slot[None] + 1, 0), 1) - 1
    weight = jnp.sum(jnp.where(hit, gate[None], 0.0), 1)
    return jnp.stack([code.astype(F32), weight])


def arrive_kernel(
    local, x, table, w_gate, w_up, s_gate, s_up, s_down,
    xs, codes, gates, h, shared,
    got, tab, ring, ring2, acc, z, hidden, stage,
    ring_sem, ring2_sem, stage_sem, cross_send, cross_recv, pass_send, pass_recv,
    own_send, own_recv, tab_send, tab_recv, out_sem,
):
    (tokens, d), ff = x.shape, s_gate.shape[1]
    chunks = d // KB
    me = lax.axis_index("ep")
    partner, across = me + 1 - 2 * lax.rem(me, 2), lax.rem(me + 2, 4)
    peers = (partner, across, 3 - me)

    barrier = pltpu.get_barrier_semaphore()
    for peer in peers:
        pl.semaphore_signal(
            barrier, inc=1, device_id={"ep": peer}, device_id_type=pl.DeviceIdType.MESH
        )
    pl.semaphore_wait(barrier, 3)

    def remote(src, dst, send, recv, peer):
        return pltpu.make_async_remote_copy(
            src, dst, send, recv, device_id={"ep": peer}, device_id_type=pl.DeviceIdType.MESH
        )

    def columns(k):
        return pl.ds(pl.multiple_of(k * KB, KB), KB)

    def cross(k):
        c = columns(k)
        return remote(x.at[:, c], got.at[1, :, c], cross_send.at[k], cross_recv.at[k], across)

    def onward(k):
        c = columns(k)
        return remote(
            got.at[1, :, c], got.at[2, :, c], pass_send.at[k], pass_recv.at[k], partner
        )

    own = remote(x, got.at[0], own_send, own_recv, partner)
    tab_copies = [
        remote(table, tab.at[i], tab_send.at[i], tab_recv.at[i], peer)
        for i, peer in enumerate(peers)
    ]

    def keep(i, k):
        c = columns(k)
        return pltpu.make_async_copy(got.at[i, :, c], xs.at[i, :, c], out_sem.at[i, k])

    n_shared = 2 * chunks
    n_all = n_shared + 2 * EARLY * chunks
    slots = ring.shape[0]

    def fetch(j):
        slot = lax.rem(j, slots)

        def go(src):
            pltpu.make_async_copy(src, ring.at[slot], ring_sem.at[slot]).start()

        for i, w in enumerate((s_gate, s_up)):

            @pl.when((j < n_shared) & (lax.rem(j, 2) == i))
            def _(w=w):
                go(w.at[columns(j // 2), :])

        i = jnp.maximum(j - n_shared, 0)
        k, q = i // (2 * EARLY), lax.rem(i, 2 * EARLY)
        for s, w in enumerate((w_gate, w_up)):

            @pl.when((j >= n_shared) & (j < n_all) & (lax.rem(q, 2) == s))
            def _(w=w):
                go(w.at[q // 2, columns(k), :])

    def ready(j):
        slot = lax.rem(j, slots)
        pltpu.make_async_copy(s_gate.at[:KB, :], ring.at[slot], ring_sem.at[slot]).wait()
        return slot

    wide = ring2.shape[2]

    deep = ring2.shape[0]

    def down_tile(n):
        slot = lax.rem(n, deep)
        c = pl.ds(pl.multiple_of(n * wide, wide), wide)
        return pltpu.make_async_copy(s_down.at[:, c], ring2.at[slot], ring2_sem.at[slot])

    def put(n):
        slot = lax.rem(n, 2)
        c = pl.ds(pl.multiple_of(n * wide, wide), wide)
        return pltpu.make_async_copy(stage.at[slot], shared.at[:, c], stage_sem.at[slot])

    for copy in tab_copies:
        copy.start()

    @pl.loop(0, chunks)
    def _(k):
        cross(k).start()

    own.start()
    for j in range(slots):
        fetch(jnp.int32(j))
    for n in range(deep):
        down_tile(jnp.int32(n)).start()

    @pl.loop(0, n_shared)
    def _(j):
        slot = ready(j)
        a = x[:, columns(j // 2)]
        side = lax.rem(j, 2)
        for n in range(ff // 512):
            c = slice(n * 512, n * 512 + 512)
            old = jnp.where(j < 2, 0.0, acc[side, :tokens, c])
            acc[side, :tokens, c] = old + dot(a, ring[slot, :, c])
        fetch(j + slots)

    for n in range(ff // 512):
        c = slice(n * 512, n * 512 + 512)
        hidden[:, c] = (silu(acc[0, :tokens, c]) * acc[1, :tokens, c]).astype(BF16)

    def pass_on(k):
        cross(k).wait_recv()
        onward(k).start()
        keep(0, k).start()
        keep(1, k).start()

    own.wait()
    pass_on(jnp.int32(0))
    n_down = d // wide

    @pl.loop(0, n_down)
    def _(n):
        down_tile(n).wait()

        @pl.when(n >= 2)
        def _():
            put(n - 2).wait()

        slot = lax.rem(n, 2)
        stage[slot] = dot(hidden[...], ring2[lax.rem(n, deep)])

        @pl.when(n + deep < n_down)
        def _():
            down_tile(n + deep).start()

        put(n).start()

    put(n_down - 2).wait()
    put(n_down - 1).wait()

    for copy in tab_copies:
        copy.wait()
    for e in range(local):
        for i in range(4):
            t = table if i == 0 else tab.at[i - 1]
            row = pl.ds(me * local + e, 1)
            codes[e, i : i + 1, :] = t[0, row, :]
            gates[e, i : i + 1, :] = t[1, row, :]

    rows = lax.broadcasted_iota(jnp.int32, (STEP, 256), 0).astype(F32)

    @pl.loop(0, chunks)
    def _(k):
        c = columns(k)
        def picked(i, a):
            parts = []
            for e in range(EARLY):
                parts.append((rows == codes[e, i : i + 1, :]).astype(BF16))
            z_i = dot(jnp.concatenate(parts, 0), a).astype(BF16)
            for e in range(EARLY):
                z[e, i * STEP : (i + 1) * STEP, :] = z_i[e * STEP : (e + 1) * STEP, :]

        picked(0, x[:, c])
        picked(1, got[0, :, c])
        picked(2, got[1, :, c])
        onward(k).wait_recv()
        keep(2, k).start()
        picked(3, got[2, :, c])

        @pl.loop(0, 2 * EARLY)
        def _(q):
            j = n_shared + 2 * EARLY * k + q
            slot = ready(j)

            @pl.when((q == EARLY) & (k + 1 < chunks))
            def _():
                pass_on(k + 1)

            for n in range(ff // 512):
                cc = slice(n * 512, n * 512 + 512)
                old = jnp.where(k == 0, 0.0, acc[q, :, cc])
                acc[q, :, cc] = old + dot(z[q // 2], ring[slot, :, cc])
            fetch(j + slots)

    for e in range(EARLY):
        for n in range(ff // 512):
            c = slice(n * 512, n * 512 + 512)
            g, u = acc[2 * e, :, c], acc[2 * e + 1, :, c]
            h[e, :, c] = (silu(g) * u).astype(BF16)

    @pl.loop(0, chunks)
    def _(k):
        cross(k).wait_send()
        onward(k).wait_send()
        for i in range(3):
            keep(i, k).wait()


def arrive(x, table, w_gate, w_up, s_gate, s_up, s_down):
    tokens, d = x.shape
    local, _, ff = w_gate.shape
    chunks = d // KB
    vmem, hbm = pl.BlockSpec(memory_space=pltpu.VMEM), pl.BlockSpec(memory_space=pl.ANY)
    dma = pltpu.SemaphoreType.DMA
    return pl.pallas_call(
        functools.partial(arrive_kernel, local),
        in_specs=[vmem] * 2 + [hbm] * 5,
        out_specs=[hbm, vmem, vmem, vmem, hbm],
        out_shape=[
            jax.ShapeDtypeStruct((3, tokens, d), BF16),
            jax.ShapeDtypeStruct((local, 4, tokens), F32),
            jax.ShapeDtypeStruct((local, 4, tokens), F32),
            jax.ShapeDtypeStruct((EARLY, 4 * STEP, ff), BF16),
            jax.ShapeDtypeStruct((tokens, d), F32),
        ],
        scratch_shapes=[
            pltpu.VMEM((3, tokens, d), BF16),
            pltpu.VMEM((3, *table.shape), F32),
            pltpu.VMEM((3, KB, ff), BF16),
            pltpu.VMEM((4, ff, 512), BF16),
            pltpu.VMEM((2 * EARLY, 4 * STEP, ff), F32),
            pltpu.VMEM((EARLY, 4 * STEP, KB), BF16),
            pltpu.VMEM((tokens, ff), BF16),
            pltpu.VMEM((2, tokens, 512), F32),
            dma((3,)), dma((4,)), dma((2,)),
            dma((chunks,)), dma((chunks,)), dma((chunks,)), dma((chunks,)),
            dma, dma, dma((3,)), dma((3,)), dma((3, chunks)),
        ],
        compiler_params=pltpu.CompilerParams(
            collective_id=0, has_side_effects=True, vmem_limit_bytes=VMEM
        ),
        name="arrive",
    )(x, table, w_gate, w_up, s_gate, s_up, s_down)


def up_kernel(block, meta, code, x0, x1, wg, wu, h_out, z, packed, gated):
    depth = x0.shape[1]
    e, n = pl.program_id(0), pl.program_id(1)
    at_meta = (e + EARLY) * 8
    total = pl.multiple_of(meta[at_meta + 4], 16)

    @pl.when(n == 0)
    def _():
        rows = lax.broadcasted_iota(jnp.int32, (STEP, 256), 0).astype(F32)
        picks = [(rows == code[0, k : k + 1, :]).astype(BF16) for k in range(4)]

        @pl.loop(0, depth // 1792)
        def _(c):
            cols = pl.ds(pl.multiple_of(c * 1792, 256), 1792)
            parts = [
                dot(picks[k], x0[:, cols] if k == 0 else x1[k - 1, :, cols]).astype(BF16)
                for k in range(4)
            ]
            for k in range(4):
                at = pl.multiple_of(meta[at_meta + k], 16)
                z[pl.ds(at, STEP), cols] = parts[k]

        z[pl.ds(total, STEP), :] = jnp.zeros((STEP, depth), BF16)

    size = (total + STEP - 1) // STEP
    @pl.when(size == 0)
    def _():
        h_out[...] = jnp.zeros_like(h_out)

    for v in range(1, 5):

        @pl.when(size == v)
        def _(v=v):
            m = v * STEP
            gated[:m, :] = silu(dot(z[:m, :], wg[0]))
            u = dot(z[:m, :], wu[0])
            packed[:m, :] = (gated[:m, :] * u).astype(BF16)
            packed[m : m + STEP, :] = jnp.zeros((STEP, block), BF16)
            for k in range(4):
                at = pl.multiple_of(meta[at_meta + k], 16)
                h_out[0, k * STEP : (k + 1) * STEP, :] = packed[pl.ds(at, STEP), :]


def up(meta, code, x0, x1, w_gate, w_up, block):
    experts, depth, ff = w_gate.shape
    late = experts - EARLY
    once = pl.Buffered(1)
    weight = pl.BlockSpec((1, depth, block), lambda e, n, m: (e + EARLY, 0, n))
    return pl.pallas_call(
        functools.partial(up_kernel, block),
        grid_spec=pltpu.PrefetchScalarGridSpec(
            num_scalar_prefetch=1,
            grid=(late, ff // block),
            in_specs=[
                pl.BlockSpec((1, 4, 256), lambda e, n, m: (e + EARLY, 0, 0)),
                pl.BlockSpec((256, depth), lambda e, n, m: (0, 0), pipeline_mode=once),
                pl.BlockSpec((3, 256, depth), lambda e, n, m: (0, 0, 0), pipeline_mode=once),
                weight,
                weight,
            ],
            out_specs=pl.BlockSpec((1, 4 * STEP, block), lambda e, n, m: (e, 0, n)),
            scratch_shapes=[
                pltpu.VMEM((5 * STEP, depth), BF16),
                pltpu.VMEM((5 * STEP, block), BF16),
                pltpu.VMEM((4 * STEP, block), F32),
            ],
        ),
        out_shape=jax.ShapeDtypeStruct((late, 4 * STEP, ff), BF16),
        compiler_params=pltpu.CompilerParams(
            vmem_limit_bytes=VMEM, dimension_semantics=("arbitrary", "arbitrary")
        ),
        cost_estimate=pl.CostEstimate(
            flops=late * 300 * depth * ff * 4,
            bytes_accessed=late * depth * ff * 4,
            transcendentals=0,
        ),
        name="up",
    )(meta, code, x0, x1, w_gate, w_up)


def finish_kernel(
    chunks, code, gate, early, late, wd, shared, y,
    h, wt, stack, own, far, near, near_got, out, out_got,
    sem, near_send, near_recv, out_send, out_recv,
):
    experts, block = wd.shape[0], wd.shape[2]
    i = pl.program_id(0)
    me = lax.axis_index("ep")
    partner, across = me + 1 - 2 * lax.rem(me, 2), lax.rem(me + 2, 4)

    def remote(src, dst, send, recv, peer):
        return pltpu.make_async_remote_copy(
            src, dst, send, recv, device_id={"ep": peer}, device_id_type=pl.DeviceIdType.MESH
        )

    def to_partner(j):
        return remote(
            near.at[lax.rem(j, 2)], near_got.at[j], near_send.at[lax.rem(j, 2)], near_recv.at[j],
            partner,
        )

    def to_across(j):
        return remote(
            out.at[lax.rem(j, 2)], out_got.at[j], out_send.at[lax.rem(j, 2)], out_recv.at[j],
            across,
        )

    def load(e):
        src = early.at[e] if e < EARLY else late.at[e - EARLY]
        return pltpu.make_async_copy(src, h.at[e], sem.at[e])

    @pl.when(i == 0)
    def _():
        barrier = pltpu.get_barrier_semaphore()
        for peer in (partner, across):
            pl.semaphore_signal(
                barrier, inc=1, device_id={"ep": peer}, device_id_type=pl.DeviceIdType.MESH
            )
        for e in range(experts):
            load(e).start()
        stack[...] = jnp.zeros_like(stack)
        rows = lax.broadcasted_iota(jnp.int32, (STEP, 256), 0).astype(F32)
        for k in range(4):
            parts = [
                jnp.where(rows == code[e, k : k + 1, :], gate[e, k : k + 1, :], 0.0)
                for e in range(experts)
            ]
            parts.append(jnp.zeros((stack.shape[1] - experts * STEP, 256), F32))
            wt[k] = jnp.concatenate(parts, 0).T.astype(BF16)
        for e in range(experts // 2):
            load(e).wait()
        pl.semaphore_wait(barrier, 2)

    @pl.when(i >= 3)
    def _():
        j = i - 3
        to_across(j).wait_recv()
        total = own[lax.rem(j, 4)] + near_got[j, 0].astype(F32) + out_got[j].astype(F32)
        y[...] = (total + shared[...]).astype(BF16)

    def make(e):
        made = dot(h[e], wd[e]).astype(BF16)
        for k in range(4):
            stack[k, e * STEP : (e + 1) * STEP, :] = made[k * STEP : (k + 1) * STEP, :]

    half = experts // 2

    @pl.when(i < chunks)
    def _():
        for e in range(half):
            make(e)

    @pl.when((i >= 1) & (i <= chunks))
    def _():
        j = i - 1

        @pl.when(j >= 2)
        def _():
            to_across(j - 2).wait_send()

        to_partner(j).wait_recv()
        out[lax.rem(j, 2)] = (far[...] + near_got[j, 1].astype(F32)).astype(BF16)
        to_across(j).start()

    @pl.when(i == 0)
    def _():
        for e in range(half, experts):
            load(e).wait()

    @pl.when(i < chunks)
    def _():
        for e in range(half, experts):
            make(e)

        @pl.when(i >= 2)
        def _():
            to_partner(i - 2).wait_send()

        slot = lax.rem(i, 2)
        near[slot, 1] = dot(wt[3], stack[3]).astype(BF16)
        near[slot, 0] = dot(wt[1], stack[1]).astype(BF16)
        far[...] = dot(wt[2], stack[2])
        to_partner(i).start()
        own[lax.rem(i, 4)] = dot(wt[0], stack[0])

    @pl.when(i == chunks + 2)
    def _():
        for j in (chunks - 2, chunks - 1):
            to_partner(j).wait_send()
            to_across(j).wait_send()


def finish(code, gate, early, late, w_down, shared, block):
    experts, ff, d = w_down.shape
    chunks = d // block
    once = pl.Buffered(1)
    small = pl.BlockSpec((experts, 4, 256), lambda i: (0, 0, 0), pipeline_mode=once)
    result = pl.BlockSpec((256, block), lambda i: (0, jnp.maximum(i - 3, 0)))
    depth = -(-experts * STEP // 256) * 256
    dma = pltpu.SemaphoreType.DMA
    return pl.pallas_call(
        functools.partial(finish_kernel, chunks),
        grid=(chunks + 3,),
        in_specs=[
            small,
            small,
            pl.BlockSpec(memory_space=pl.ANY),
            pl.BlockSpec(memory_space=pl.ANY),
            pl.BlockSpec((experts, ff, block), lambda i: (0, 0, jnp.minimum(i, chunks - 1))),
            result,
        ],
        out_specs=result,
        scratch_shapes=[
            pltpu.VMEM((experts, 4 * STEP, ff), BF16),
            pltpu.VMEM((4, 256, depth), BF16),
            pltpu.VMEM((4, depth, block), BF16),
            pltpu.VMEM((4, 256, block), F32),
            pltpu.VMEM((256, block), F32),
            pltpu.VMEM((2, 2, 256, block), BF16),
            pltpu.VMEM((chunks, 2, 256, block), BF16),
            pltpu.VMEM((2, 256, block), BF16),
            pltpu.VMEM((chunks, 256, block), BF16),
            dma((experts,)),
            dma((2,)),
            dma((chunks,)),
            dma((2,)),
            dma((chunks,)),
        ],
        out_shape=jax.ShapeDtypeStruct((256, d), BF16),
        compiler_params=pltpu.CompilerParams(
            collective_id=1,
            has_side_effects=True,
            vmem_limit_bytes=VMEM,
            dimension_semantics=("arbitrary",),
        ),
        name="finish",
    )(code, gate, early, late, w_down, shared)


def layer(x, expert, slot, gate, w_gate, w_up, w_down, s_gate, s_up, s_down):
    local = w_gate.shape[0]
    experts = 4 * local
    x, expert, slot, gate = x[0, 0], expert[0, 0], slot[0, 0], gate[0, 0]
    tokens, top = expert.shape
    slots = 5 * tokens * top // (4 * experts)
    table = tables(expert, slot, gate, experts, slots)
    xs, code, weight, early, shared = arrive(x, table, w_gate, w_up, s_gate, s_up, s_down)
    used = (jnp.max(code, -1).astype(jnp.int32) + 16) // 16 * 16
    starts = [jnp.zeros_like(used[:, 0])]
    for k in range(4):
        starts.append(starts[-1] + used[:, k])
    meta = jnp.stack(starts + starts[:3], 1).reshape(-1)

    late = up(meta, code, x, xs, w_gate, w_up, 512)
    return finish(code, weight, early, late, w_down, shared, 512)[None, None]


def solution(mesh):
    rows, whole = P("dp", "ep"), P()
    return jax.shard_map(
        layer,
        mesh=mesh,
        in_specs=(rows,) * 4 + (P("ep"),) * 3 + (whole,) * 3,
        out_specs=rows,
        check_vma=False,
    )
```

```python
import functools

import jax
import jax.numpy as jnp
from jax import lax
from jax.experimental import pallas as pl
from jax.experimental.pallas import tpu as pltpu
from jax.sharding import PartitionSpec as P

STEP = 112
EARLY = 2
VMEM = 63 * 2**20
KB = 1024
F32, BF16 = jnp.float32, jnp.bfloat16


def silu(g):
    return g / (1.0 + jnp.exp(-g))


def dot(a, b):
    return jnp.dot(a, b, preferred_element_type=F32)


def tables(expert, slot, gate, experts, slots):
    expert, slot, gate = expert.T, slot.T, gate.T
    hit = (expert[None] == jnp.arange(experts)[:, None, None]) & (slot < slots)[None]
    code = jnp.sum(jnp.where(hit, slot[None] + 1, 0), 1) - 1
    weight = jnp.sum(jnp.where(hit, gate[None], 0.0), 1)
    return jnp.stack([code.astype(F32), weight])


def arrive_kernel(
    local, x, table, w_gate, w_up, s_gate, s_up, s_down,
    xs, codes, gates, h, shared,
    got, tab, ring, ring2, acc, z, hidden, stage,
    ring_sem, ring2_sem, stage_sem, cross_send, cross_recv, pass_send, pass_recv,
    own_send, own_recv, tab_send, tab_recv, out_sem,
):
    (tokens, d), ff = x.shape, s_gate.shape[1]
    chunks = d // KB
    me = lax.axis_index("ep")
    partner, across = me + 1 - 2 * lax.rem(me, 2), lax.rem(me + 2, 4)
    peers = (partner, across, 3 - me)

    barrier = pltpu.get_barrier_semaphore()
    for peer in peers:
        pl.semaphore_signal(
            barrier, inc=1, device_id={"ep": peer}, device_id_type=pl.DeviceIdType.MESH
        )
    pl.semaphore_wait(barrier, 3)

    def remote(src, dst, send, recv, peer):
        return pltpu.make_async_remote_copy(
            src, dst, send, recv, device_id={"ep": peer}, device_id_type=pl.DeviceIdType.MESH
        )

    def columns(k):
        return pl.ds(pl.multiple_of(k * KB, KB), KB)

    def cross(k):
        c = columns(k)
        return remote(x.at[:, c], got.at[1, :, c], cross_send.at[k], cross_recv.at[k], across)

    def onward(k):
        c = columns(k)
        return remote(
            got.at[1, :, c], got.at[2, :, c], pass_send.at[k], pass_recv.at[k], partner
        )

    own = remote(x, got.at[0], own_send, own_recv, partner)
    tab_copies = [
        remote(table, tab.at[i], tab_send.at[i], tab_recv.at[i], peer)
        for i, peer in enumerate(peers)
    ]

    def keep(i, k):
        c = columns(k)
        return pltpu.make_async_copy(got.at[i, :, c], xs.at[i, :, c], out_sem.at[i, k])

    n_shared = 2 * chunks
    n_all = n_shared + 2 * EARLY * chunks
    slots = ring.shape[0]

    def fetch(j):
        slot = lax.rem(j, slots)

        def go(src):
            pltpu.make_async_copy(src, ring.at[slot], ring_sem.at[slot]).start()

        for i, w in enumerate((s_gate, s_up)):

            @pl.when((j < n_shared) & (lax.rem(j, 2) == i))
            def _(w=w):
                go(w.at[columns(j // 2), :])

        i = jnp.maximum(j - n_shared, 0)
        k, q = i // (2 * EARLY), lax.rem(i, 2 * EARLY)
        for s, w in enumerate((w_gate, w_up)):

            @pl.when((j >= n_shared) & (j < n_all) & (lax.rem(q, 2) == s))
            def _(w=w):
                go(w.at[q // 2, columns(k), :])

    def ready(j):
        slot = lax.rem(j, slots)
        pltpu.make_async_copy(s_gate.at[:KB, :], ring.at[slot], ring_sem.at[slot]).wait()
        return slot

    wide = ring2.shape[2]

    deep = ring2.shape[0]

    def down_tile(n):
        slot = lax.rem(n, deep)
        c = pl.ds(pl.multiple_of(n * wide, wide), wide)
        return pltpu.make_async_copy(s_down.at[:, c], ring2.at[slot], ring2_sem.at[slot])

    def put(n):
        slot = lax.rem(n, 2)
        c = pl.ds(pl.multiple_of(n * wide, wide), wide)
        return pltpu.make_async_copy(stage.at[slot], shared.at[:, c], stage_sem.at[slot])

    for copy in tab_copies:
        copy.start()

    @pl.loop(0, chunks)
    def _(k):
        cross(k).start()

    own.start()
    for j in range(slots):
        fetch(jnp.int32(j))
    for n in range(deep):
        down_tile(jnp.int32(n)).start()

    @pl.loop(0, n_shared)
    def _(j):
        slot = ready(j)
        a = x[:, columns(j // 2)]
        side = lax.rem(j, 2)
        for n in range(ff // 512):
            c = slice(n * 512, n * 512 + 512)
            old = jnp.where(j < 2, 0.0, acc[side, :tokens, c])
            acc[side, :tokens, c] = old + dot(a, ring[slot, :, c])
        fetch(j + slots)

    for n in range(ff // 512):
        c = slice(n * 512, n * 512 + 512)
        hidden[:, c] = (silu(acc[0, :tokens, c]) * acc[1, :tokens, c]).astype(BF16)

    def pass_on(k):
        cross(k).wait_recv()
        onward(k).start()
        keep(0, k).start()
        keep(1, k).start()

    own.wait()
    pass_on(jnp.int32(0))
    n_down = d // wide

    @pl.loop(0, n_down)
    def _(n):
        down_tile(n).wait()

        @pl.when(n >= 2)
        def _():
            put(n - 2).wait()

        slot = lax.rem(n, 2)
        stage[slot] = dot(hidden[...], ring2[lax.rem(n, deep)])

        @pl.when(n + deep < n_down)
        def _():
            down_tile(n + deep).start()

        put(n).start()

    put(n_down - 2).wait()
    put(n_down - 1).wait()

    for copy in tab_copies:
        copy.wait()
    for e in range(local):
        for i in range(4):
            t = table if i == 0 else tab.at[i - 1]
            row = pl.ds(me * local + e, 1)
            codes[e, i : i + 1, :] = t[0, row, :]
            gates[e, i : i + 1, :] = t[1, row, :]

    rows = lax.broadcasted_iota(jnp.int32, (STEP, 256), 0).astype(F32)

    @pl.loop(0, chunks)
    def _(k):
        c = columns(k)
        def picked(i, a):
            parts = []
            for e in range(EARLY):
                parts.append((rows == codes[e, i : i + 1, :]).astype(BF16))
            z_i = dot(jnp.concatenate(parts, 0), a).astype(BF16)
            for e in range(EARLY):
                z[e, i * STEP : (i + 1) * STEP, :] = z_i[e * STEP : (e + 1) * STEP, :]

        picked(0, x[:, c])
        picked(1, got[0, :, c])
        picked(2, got[1, :, c])
        onward(k).wait_recv()
        keep(2, k).start()
        picked(3, got[2, :, c])

        @pl.loop(0, 2 * EARLY)
        def _(q):
            j = n_shared + 2 * EARLY * k + q
            slot = ready(j)

            @pl.when((q == EARLY) & (k + 1 < chunks))
            def _():
                pass_on(k + 1)

            for n in range(ff // 512):
                cc = slice(n * 512, n * 512 + 512)
                old = jnp.where(k == 0, 0.0, acc[q, :, cc])
                acc[q, :, cc] = old + dot(z[q // 2], ring[slot, :, cc])
            fetch(j + slots)

    for e in range(EARLY):
        for n in range(ff // 512):
            c = slice(n * 512, n * 512 + 512)
            g, u = acc[2 * e, :, c], acc[2 * e + 1, :, c]
            h[e, :, c] = (silu(g) * u).astype(BF16)

    @pl.loop(0, chunks)
    def _(k):
        cross(k).wait_send()
        onward(k).wait_send()
        for i in range(3):
            keep(i, k).wait()


def arrive(x, table, w_gate, w_up, s_gate, s_up, s_down):
    tokens, d = x.shape
    local, _, ff = w_gate.shape
    chunks = d // KB
    vmem, hbm = pl.BlockSpec(memory_space=pltpu.VMEM), pl.BlockSpec(memory_space=pl.ANY)
    dma = pltpu.SemaphoreType.DMA
    return pl.pallas_call(
        functools.partial(arrive_kernel, local),
        in_specs=[vmem] * 2 + [hbm] * 5,
        out_specs=[hbm, vmem, vmem, vmem, hbm],
        out_shape=[
            jax.ShapeDtypeStruct((3, tokens, d), BF16),
            jax.ShapeDtypeStruct((local, 4, tokens), F32),
            jax.ShapeDtypeStruct((local, 4, tokens), F32),
            jax.ShapeDtypeStruct((EARLY, 4 * STEP, ff), BF16),
            jax.ShapeDtypeStruct((tokens, d), F32),
        ],
        scratch_shapes=[
            pltpu.VMEM((3, tokens, d), BF16),
            pltpu.VMEM((3, *table.shape), F32),
            pltpu.VMEM((3, KB, ff), BF16),
            pltpu.VMEM((4, ff, 512), BF16),
            pltpu.VMEM((2 * EARLY, 4 * STEP, ff), F32),
            pltpu.VMEM((EARLY, 4 * STEP, KB), BF16),
            pltpu.VMEM((tokens, ff), BF16),
            pltpu.VMEM((2, tokens, 512), F32),
            dma((3,)), dma((4,)), dma((2,)),
            dma((chunks,)), dma((chunks,)), dma((chunks,)), dma((chunks,)),
            dma, dma, dma((3,)), dma((3,)), dma((3, chunks)),
        ],
        compiler_params=pltpu.CompilerParams(
            collective_id=0, has_side_effects=True, vmem_limit_bytes=VMEM
        ),
        name="arrive",
    )(x, table, w_gate, w_up, s_gate, s_up, s_down)


def up_kernel(
    meta, code, x0, xs, w_gate, w_up, h_out,
    z, part, ring, packed, piece, part_sem, ring_sem, piece_sem,
):
    late, depth = code.shape[0] - EARLY, x0.shape[1]
    slots, block = ring.shape[0], ring.shape[2] // 2
    n_jobs = late * w_gate.shape[2] // block
    width = part.shape[3]

    def begin(e, k):
        return pl.multiple_of(meta[(e + EARLY) * 8 + k], 16)

    def fetches(j):
        e, slot = lax.rem(j, late) + EARLY, lax.rem(j, slots)
        c = pl.ds(pl.multiple_of((j // late) * block, block), block)
        return [
            pltpu.make_async_copy(
                w.at[e, :, c], ring.at[slot, :, pl.ds(i * block, block)], ring_sem.at[slot, i]
            )
            for i, w in enumerate((w_gate, w_up))
        ]

    def columns(c):
        return pl.ds(pl.multiple_of(c * width, width), width)

    def tokens(c):
        at = lax.rem(c, 2)
        return [
            pltpu.make_async_copy(x0.at[:, columns(c)], part.at[at, 0], part_sem.at[at, 0]),
            pltpu.make_async_copy(
                xs.at[:, :, columns(c)], part.at[at, pl.ds(1, 3)], part_sem.at[at, 1]
            ),
        ]

    for c in range(2):
        for copy in tokens(jnp.int32(c)):
            copy.start()
    for j in range(slots):
        for copy in fetches(jnp.int32(j)):
            copy.start()

    rows = lax.broadcasted_iota(jnp.int32, (STEP, 256), 0).astype(F32)
    picks = [
        jnp.concatenate(
            [(rows == code[e + EARLY, k : k + 1, :]).astype(BF16) for e in range(late)], 0
        )
        for k in range(4)
    ]

    @pl.loop(0, depth // width)
    def _(c):
        for copy in tokens(c):
            copy.wait()
        for e in range(late):
            at = pl.multiple_of(e * 4 * STEP + begin(e, 4), 16)
            z[pl.ds(at, STEP), columns(c)] = jnp.zeros((STEP, width), BF16)
        for k in range(4):
            got = dot(picks[k], part[lax.rem(c, 2), k]).astype(BF16)
            for e in range(late):
                at = pl.multiple_of(e * 4 * STEP + begin(e, k), 16)
                z[pl.ds(at, STEP), columns(c)] = got[e * STEP : (e + 1) * STEP, :]

        @pl.when(c + 2 < depth // width)
        def _():
            for copy in tokens(c + 2):
                copy.start()

    def put(j):
        c = pl.ds(pl.multiple_of((j // late) * block, block), block)
        at = lax.rem(j, 2)
        return pltpu.make_async_copy(
            piece.at[at], h_out.at[lax.rem(j, late), :, c], piece_sem.at[at]
        )

    @pl.loop(0, n_jobs)
    def _(j):
        e, slot = lax.rem(j, late), lax.rem(j, slots)
        for copy in fetches(j):
            copy.wait()
        size = (begin(e, 4) + STEP - 1) // STEP

        @pl.when(size == 0)
        def _():
            packed[...] = jnp.zeros_like(packed)

        for v in range(1, 5):

            @pl.when(size == v)
            def _(v=v):
                m = v * STEP
                first = pl.multiple_of(e * 4 * STEP, 16)
                both = dot(z[pl.ds(first, m), :], ring[slot])
                packed[:m, :] = (silu(both[:, :block]) * both[:, block:]).astype(BF16)
                packed[m : m + STEP, :] = jnp.zeros((STEP, block), BF16)

        @pl.when(j + slots < n_jobs)
        def _():
            for copy in fetches(j + slots):
                copy.start()

        @pl.when(j >= 2)
        def _():
            put(j - 2).wait()

        for k in range(4):
            piece[lax.rem(j, 2), k * STEP : (k + 1) * STEP, :] = packed[pl.ds(begin(e, k), STEP), :]
        put(j).start()

    put(jnp.int32(n_jobs - 2)).wait()
    put(jnp.int32(n_jobs - 1)).wait()


def up(meta, code, x0, xs, w_gate, w_up, block):
    experts, depth, ff = w_gate.shape
    late = experts - EARLY
    hbm, dma = pl.BlockSpec(memory_space=pl.ANY), pltpu.SemaphoreType.DMA
    return pl.pallas_call(
        up_kernel,
        in_specs=[
            pl.BlockSpec(memory_space=pltpu.SMEM),
            pl.BlockSpec(memory_space=pltpu.VMEM),
            hbm, hbm, hbm, hbm,
        ],
        out_specs=hbm,
        scratch_shapes=[
            pltpu.VMEM(((4 * late + 1) * STEP, depth), BF16),
            pltpu.VMEM((2, 4, 256, 1024), BF16),
            pltpu.VMEM((3, depth, 2 * block), BF16),
            pltpu.VMEM((5 * STEP, block), BF16),
            pltpu.VMEM((2, 4 * STEP, block), BF16),
            dma((2, 2)), dma((3, 2)), dma((2,)),
        ],
        out_shape=jax.ShapeDtypeStruct((late, 4 * STEP, ff), BF16),
        compiler_params=pltpu.CompilerParams(vmem_limit_bytes=VMEM),
        cost_estimate=pl.CostEstimate(
            flops=late * 300 * depth * ff * 4,
            bytes_accessed=late * depth * ff * 4,
            transcendentals=0,
        ),
        name="up",
    )(meta, code, x0, xs, w_gate, w_up)


def finish_kernel(
    chunks, code, gate, early, late, wd, shared, y,
    h, wt, stack, own, far, near, near_got, out, out_got,
    sem, near_send, near_recv, out_send, out_recv,
):
    experts, block = wd.shape[0], wd.shape[2]
    i = pl.program_id(0)
    me = lax.axis_index("ep")
    partner, across = me + 1 - 2 * lax.rem(me, 2), lax.rem(me + 2, 4)

    def remote(src, dst, send, recv, peer):
        return pltpu.make_async_remote_copy(
            src, dst, send, recv, device_id={"ep": peer}, device_id_type=pl.DeviceIdType.MESH
        )

    def to_partner(j):
        return remote(
            near.at[lax.rem(j, 2)], near_got.at[j], near_send.at[lax.rem(j, 2)], near_recv.at[j],
            partner,
        )

    def to_across(j):
        return remote(
            out.at[lax.rem(j, 2)], out_got.at[j], out_send.at[lax.rem(j, 2)], out_recv.at[j],
            across,
        )

    def load(e):
        src = early.at[e] if e < EARLY else late.at[e - EARLY]
        return pltpu.make_async_copy(src, h.at[e], sem.at[e])

    @pl.when(i == 0)
    def _():
        barrier = pltpu.get_barrier_semaphore()
        for peer in (partner, across):
            pl.semaphore_signal(
                barrier, inc=1, device_id={"ep": peer}, device_id_type=pl.DeviceIdType.MESH
            )
        for e in range(experts):
            load(e).start()
        stack[...] = jnp.zeros_like(stack)
        rows = lax.broadcasted_iota(jnp.int32, (STEP, 256), 0).astype(F32)
        for k in range(4):
            parts = [
                jnp.where(rows == code[e, k : k + 1, :], gate[e, k : k + 1, :], 0.0)
                for e in range(experts)
            ]
            parts.append(jnp.zeros((stack.shape[1] - experts * STEP, 256), F32))
            wt[k] = jnp.concatenate(parts, 0).T.astype(BF16)
        for e in range(experts // 2):
            load(e).wait()
        pl.semaphore_wait(barrier, 2)

    @pl.when(i >= 3)
    def _():
        j = i - 3
        to_across(j).wait_recv()
        total = own[lax.rem(j, 4)] + near_got[j, 0].astype(F32) + out_got[j].astype(F32)
        y[...] = (total + shared[...]).astype(BF16)

    def make(e):
        made = dot(h[e], wd[e]).astype(BF16)
        for k in range(4):
            stack[k, e * STEP : (e + 1) * STEP, :] = made[k * STEP : (k + 1) * STEP, :]

    half = experts // 2

    @pl.when(i < chunks)
    def _():
        for e in range(half):
            make(e)

    @pl.when((i >= 1) & (i <= chunks))
    def _():
        j = i - 1

        @pl.when(j >= 2)
        def _():
            to_across(j - 2).wait_send()

        to_partner(j).wait_recv()
        out[lax.rem(j, 2)] = (far[...] + near_got[j, 1].astype(F32)).astype(BF16)
        to_across(j).start()

    @pl.when(i == 0)
    def _():
        for e in range(half, experts):
            load(e).wait()

    @pl.when(i < chunks)
    def _():
        for e in range(half, experts):
            make(e)

        @pl.when(i >= 2)
        def _():
            to_partner(i - 2).wait_send()

        slot = lax.rem(i, 2)
        near[slot, 1] = dot(wt[3], stack[3]).astype(BF16)
        near[slot, 0] = dot(wt[1], stack[1]).astype(BF16)
        far[...] = dot(wt[2], stack[2])
        to_partner(i).start()
        own[lax.rem(i, 4)] = dot(wt[0], stack[0])

    @pl.when(i == chunks + 2)
    def _():
        for j in (chunks - 2, chunks - 1):
            to_partner(j).wait_send()
            to_across(j).wait_send()


def finish(code, gate, early, late, w_down, shared, block):
    experts, ff, d = w_down.shape
    chunks = d // block
    once = pl.Buffered(1)
    small = pl.BlockSpec((experts, 4, 256), lambda i: (0, 0, 0), pipeline_mode=once)
    result = pl.BlockSpec((256, block), lambda i: (0, jnp.maximum(i - 3, 0)))
    depth = -(-experts * STEP // 256) * 256
    dma = pltpu.SemaphoreType.DMA
    return pl.pallas_call(
        functools.partial(finish_kernel, chunks),
        grid=(chunks + 3,),
        in_specs=[
            small,
            small,
            pl.BlockSpec(memory_space=pl.ANY),
            pl.BlockSpec(memory_space=pl.ANY),
            pl.BlockSpec((experts, ff, block), lambda i: (0, 0, jnp.minimum(i, chunks - 1))),
            result,
        ],
        out_specs=result,
        scratch_shapes=[
            pltpu.VMEM((experts, 4 * STEP, ff), BF16),
            pltpu.VMEM((4, 256, depth), BF16),
            pltpu.VMEM((4, depth, block), BF16),
            pltpu.VMEM((4, 256, block), F32),
            pltpu.VMEM((256, block), F32),
            pltpu.VMEM((2, 2, 256, block), BF16),
            pltpu.VMEM((chunks, 2, 256, block), BF16),
            pltpu.VMEM((2, 256, block), BF16),
            pltpu.VMEM((chunks, 256, block), BF16),
            dma((experts,)),
            dma((2,)),
            dma((chunks,)),
            dma((2,)),
            dma((chunks,)),
        ],
        out_shape=jax.ShapeDtypeStruct((256, d), BF16),
        compiler_params=pltpu.CompilerParams(
            collective_id=1,
            has_side_effects=True,
            vmem_limit_bytes=VMEM,
            dimension_semantics=("arbitrary",),
        ),
        name="finish",
    )(code, gate, early, late, w_down, shared)


def layer(x, expert, slot, gate, w_gate, w_up, w_down, s_gate, s_up, s_down):
    local = w_gate.shape[0]
    experts = 4 * local
    x, expert, slot, gate = x[0, 0], expert[0, 0], slot[0, 0], gate[0, 0]
    tokens, top = expert.shape
    slots = 5 * tokens * top // (4 * experts)
    table = tables(expert, slot, gate, experts, slots)
    xs, code, weight, early, shared = arrive(x, table, w_gate, w_up, s_gate, s_up, s_down)
    used = (jnp.max(code, -1).astype(jnp.int32) + 16) // 16 * 16
    starts = [jnp.zeros_like(used[:, 0])]
    for k in range(4):
        starts.append(starts[-1] + used[:, k])
    meta = jnp.stack(starts + starts[:3], 1).reshape(-1)

    late = up(meta, code, x, xs, w_gate, w_up, 256)
    return finish(code, weight, early, late, w_down, shared, 512)[None, None]


def solution(mesh):
    rows, whole = P("dp", "ep"), P()
    return jax.shard_map(
        layer,
        mesh=mesh,
        in_specs=(rows,) * 4 + (P("ep"),) * 3 + (whole,) * 3,
        out_specs=rows,
        check_vma=False,
    )
```

```python
import functools

import jax
import jax.numpy as jnp
from jax import lax
from jax.experimental import pallas as pl
from jax.experimental.pallas import tpu as pltpu
from jax.sharding import PartitionSpec as P

STEP = 112
EARLY = 2
VMEM = 63 * 2**20
KB = 1024
F32, BF16 = jnp.float32, jnp.bfloat16


def silu(g):
    return g / (1.0 + jnp.exp(-g))


def dot(a, b):
    return jnp.dot(a, b, preferred_element_type=F32)


def arrive_kernel(
    local, x, expert, slot_of, gate, w_gate, w_up, s_gate, s_up, s_down,
    xs, codes, gates, h, shared,
    got, table, tab, ring, ring2, acc, z, hidden, stage,
    ring_sem, ring2_sem, stage_sem, cross_send, cross_recv, pass_send, pass_recv,
    own_send, own_recv, tab_send, tab_recv, out_sem,
):
    (tokens, d), ff = x.shape, s_gate.shape[1]
    chunks = d // KB
    me = lax.axis_index("ep")
    partner, across = me + 1 - 2 * lax.rem(me, 2), lax.rem(me + 2, 4)
    peers = (partner, across, 3 - me)

    barrier = pltpu.get_barrier_semaphore()
    for peer in peers:
        pl.semaphore_signal(
            barrier, inc=1, device_id={"ep": peer}, device_id_type=pl.DeviceIdType.MESH
        )
    pl.semaphore_wait(barrier, 3)

    def remote(src, dst, send, recv, peer):
        return pltpu.make_async_remote_copy(
            src, dst, send, recv, device_id={"ep": peer}, device_id_type=pl.DeviceIdType.MESH
        )

    def columns(k):
        return pl.ds(pl.multiple_of(k * KB, KB), KB)

    def cross(k):
        c = columns(k)
        return remote(x.at[:, c], got.at[1, :, c], cross_send.at[k], cross_recv.at[k], across)

    def onward(k):
        c = columns(k)
        return remote(
            got.at[1, :, c], got.at[2, :, c], pass_send.at[k], pass_recv.at[k], partner
        )

    own = remote(x, got.at[0], own_send, own_recv, partner)
    tab_copies = [
        remote(table, tab.at[i], tab_send.at[i], tab_recv.at[i], peer)
        for i, peer in enumerate(peers)
    ]

    def keep(i, k):
        c = columns(k)
        return pltpu.make_async_copy(got.at[i, :, c], xs.at[i, :, c], out_sem.at[i, k])

    n_shared = 2 * chunks
    n_all = n_shared + 2 * EARLY * chunks
    slots = ring.shape[0]

    def fetch(j):
        slot = lax.rem(j, slots)

        def go(src):
            pltpu.make_async_copy(src, ring.at[slot], ring_sem.at[slot]).start()

        for i, w in enumerate((s_gate, s_up)):

            @pl.when((j < n_shared) & (lax.rem(j, 2) == i))
            def _(w=w):
                go(w.at[columns(j // 2), :])

        i = jnp.maximum(j - n_shared, 0)
        k, q = i // (2 * EARLY), lax.rem(i, 2 * EARLY)
        for s, w in enumerate((w_gate, w_up)):

            @pl.when((j >= n_shared) & (j < n_all) & (lax.rem(q, 2) == s))
            def _(w=w):
                go(w.at[q // 2, columns(k), :])

    def ready(j):
        slot = lax.rem(j, slots)
        pltpu.make_async_copy(s_gate.at[:KB, :], ring.at[slot], ring_sem.at[slot]).wait()
        return slot

    wide = ring2.shape[2]

    deep = ring2.shape[0]

    def down_tile(n):
        slot = lax.rem(n, deep)
        c = pl.ds(pl.multiple_of(n * wide, wide), wide)
        return pltpu.make_async_copy(s_down.at[:, c], ring2.at[slot], ring2_sem.at[slot])

    def put(n):
        slot = lax.rem(n, 2)
        c = pl.ds(pl.multiple_of(n * wide, wide), wide)
        return pltpu.make_async_copy(stage.at[slot], shared.at[:, c], stage_sem.at[slot])

    @pl.loop(0, chunks)
    def _(k):
        cross(k).start()

    own.start()
    for j in range(slots):
        fetch(jnp.int32(j))
    for n in range(deep):
        down_tile(jnp.int32(n)).start()

    experts = 4 * local
    limit = 5 * tokens * expert.shape[0] // (4 * experts)
    kept = slot_of[...] < limit
    place = slot_of[...].astype(F32) + 1.0
    for e in range(experts):
        hit = kept & (expert[...] == e)
        table[0, e : e + 1, :] = jnp.sum(jnp.where(hit, place, 0.0), 0, keepdims=True) - 1.0
        table[1, e : e + 1, :] = jnp.sum(jnp.where(hit, gate[...], 0.0), 0, keepdims=True)

    @pl.loop(0, n_shared)
    def _(j):
        slot = ready(j)
        a = x[:, columns(j // 2)]
        side = lax.rem(j, 2)
        for n in range(ff // 512):
            c = slice(n * 512, n * 512 + 512)
            old = jnp.where(j < 2, 0.0, acc[side, :tokens, c])
            acc[side, :tokens, c] = old + dot(a, ring[slot, :, c])
        fetch(j + slots)

    for copy in tab_copies:
        copy.start()
    for n in range(ff // 512):
        c = slice(n * 512, n * 512 + 512)
        hidden[:, c] = (silu(acc[0, :tokens, c]) * acc[1, :tokens, c]).astype(BF16)

    def pass_on(k):
        cross(k).wait_recv()
        onward(k).start()
        keep(0, k).start()
        keep(1, k).start()

    own.wait()
    pass_on(jnp.int32(0))
    n_down = d // wide

    @pl.loop(0, n_down)
    def _(n):
        down_tile(n).wait()

        @pl.when(n >= 2)
        def _():
            put(n - 2).wait()

        slot = lax.rem(n, 2)
        stage[slot] = dot(hidden[...], ring2[lax.rem(n, deep)])

        @pl.when(n + deep < n_down)
        def _():
            down_tile(n + deep).start()

        put(n).start()

    put(n_down - 2).wait()
    put(n_down - 1).wait()

    for copy in tab_copies:
        copy.wait()
    for e in range(local):
        for i in range(4):
            t = table if i == 0 else tab.at[i - 1]
            row = pl.ds(me * local + e, 1)
            codes[e, i : i + 1, :] = t[0, row, :]
            gates[e, i : i + 1, :] = t[1, row, :]

    rows = lax.broadcasted_iota(jnp.int32, (STEP, 256), 0).astype(F32)

    @pl.loop(0, chunks)
    def _(k):
        c = columns(k)
        def picked(i, a):
            parts = []
            for e in range(EARLY):
                parts.append((rows == codes[e, i : i + 1, :]).astype(BF16))
            z_i = dot(jnp.concatenate(parts, 0), a).astype(BF16)
            for e in range(EARLY):
                z[e, i * STEP : (i + 1) * STEP, :] = z_i[e * STEP : (e + 1) * STEP, :]

        picked(0, x[:, c])
        picked(1, got[0, :, c])
        picked(2, got[1, :, c])
        onward(k).wait_recv()
        keep(2, k).start()
        picked(3, got[2, :, c])

        @pl.loop(0, 2 * EARLY)
        def _(q):
            j = n_shared + 2 * EARLY * k + q
            slot = ready(j)

            @pl.when((q == EARLY) & (k + 1 < chunks))
            def _():
                pass_on(k + 1)

            for n in range(ff // 512):
                cc = slice(n * 512, n * 512 + 512)
                old = jnp.where(k == 0, 0.0, acc[q, :, cc])
                acc[q, :, cc] = old + dot(z[q // 2], ring[slot, :, cc])
            fetch(j + slots)

    for e in range(EARLY):
        for n in range(ff // 512):
            c = slice(n * 512, n * 512 + 512)
            g, u = acc[2 * e, :, c], acc[2 * e + 1, :, c]
            h[e, :, c] = (silu(g) * u).astype(BF16)

    @pl.loop(0, chunks)
    def _(k):
        cross(k).wait_send()
        onward(k).wait_send()
        for i in range(3):
            keep(i, k).wait()


def arrive(x, expert, slot, gate, w_gate, w_up, s_gate, s_up, s_down):
    tokens, d = x.shape
    local, _, ff = w_gate.shape
    chunks = d // KB
    vmem, hbm = pl.BlockSpec(memory_space=pltpu.VMEM), pl.BlockSpec(memory_space=pl.ANY)
    dma = pltpu.SemaphoreType.DMA
    return pl.pallas_call(
        functools.partial(arrive_kernel, local),
        in_specs=[vmem] * 4 + [hbm] * 5,
        out_specs=[hbm, vmem, vmem, vmem, hbm],
        out_shape=[
            jax.ShapeDtypeStruct((3, tokens, d), BF16),
            jax.ShapeDtypeStruct((local, 4, tokens), F32),
            jax.ShapeDtypeStruct((local, 4, tokens), F32),
            jax.ShapeDtypeStruct((EARLY, 4 * STEP, ff), BF16),
            jax.ShapeDtypeStruct((tokens, d), F32),
        ],
        scratch_shapes=[
            pltpu.VMEM((3, tokens, d), BF16),
            pltpu.VMEM((2, 4 * local, tokens), F32),
            pltpu.VMEM((3, 2, 4 * local, tokens), F32),
            pltpu.VMEM((3, KB, ff), BF16),
            pltpu.VMEM((4, ff, 512), BF16),
            pltpu.VMEM((2 * EARLY, 4 * STEP, ff), F32),
            pltpu.VMEM((EARLY, 4 * STEP, KB), BF16),
            pltpu.VMEM((tokens, ff), BF16),
            pltpu.VMEM((2, tokens, 512), F32),
            dma((3,)), dma((4,)), dma((2,)),
            dma((chunks,)), dma((chunks,)), dma((chunks,)), dma((chunks,)),
            dma, dma, dma((3,)), dma((3,)), dma((3, chunks)),
        ],
        compiler_params=pltpu.CompilerParams(
            collective_id=0, has_side_effects=True, vmem_limit_bytes=VMEM
        ),
        name="arrive",
    )(x, expert.T, slot.T, gate.T, w_gate, w_up, s_gate, s_up, s_down)


def up_kernel(
    meta, code, x0, xs, w_gate, w_up, h_out,
    z, part, ring, packed, piece, part_sem, ring_sem, piece_sem,
):
    late, depth = code.shape[0] - EARLY, x0.shape[1]
    slots, block = ring.shape[0], ring.shape[2] // 2
    n_jobs = late * w_gate.shape[2] // block
    width = part.shape[3]

    def begin(e, k):
        return pl.multiple_of(meta[(e + EARLY) * 8 + k], 16)

    def fetches(j):
        e, slot = lax.rem(j, late) + EARLY, lax.rem(j, slots)
        c = pl.ds(pl.multiple_of((j // late) * block, block), block)
        return [
            pltpu.make_async_copy(
                w.at[e, :, c], ring.at[slot, :, pl.ds(i * block, block)], ring_sem.at[slot, i]
            )
            for i, w in enumerate((w_gate, w_up))
        ]

    def columns(c):
        return pl.ds(pl.multiple_of(c * width, width), width)

    def tokens(c):
        at = lax.rem(c, 2)
        return [
            pltpu.make_async_copy(x0.at[:, columns(c)], part.at[at, 0], part_sem.at[at, 0]),
            pltpu.make_async_copy(
                xs.at[:, :, columns(c)], part.at[at, pl.ds(1, 3)], part_sem.at[at, 1]
            ),
        ]

    for c in range(2):
        for copy in tokens(jnp.int32(c)):
            copy.start()
    for j in range(slots):
        for copy in fetches(jnp.int32(j)):
            copy.start()

    rows = lax.broadcasted_iota(jnp.int32, (STEP, 256), 0).astype(F32)
    picks = [
        jnp.concatenate(
            [(rows == code[e + EARLY, k : k + 1, :]).astype(BF16) for e in range(late)], 0
        )
        for k in range(4)
    ]

    @pl.loop(0, depth // width)
    def _(c):
        for copy in tokens(c):
            copy.wait()
        for e in range(late):
            at = pl.multiple_of(e * 4 * STEP + begin(e, 4), 16)
            z[pl.ds(at, STEP), columns(c)] = jnp.zeros((STEP, width), BF16)
        for k in range(4):
            got = dot(picks[k], part[lax.rem(c, 2), k]).astype(BF16)
            for e in range(late):
                at = pl.multiple_of(e * 4 * STEP + begin(e, k), 16)
                z[pl.ds(at, STEP), columns(c)] = got[e * STEP : (e + 1) * STEP, :]

        @pl.when(c + 2 < depth // width)
        def _():
            for copy in tokens(c + 2):
                copy.start()

    def put(j):
        c = pl.ds(pl.multiple_of((j // late) * block, block), block)
        at = lax.rem(j, 2)
        return pltpu.make_async_copy(
            piece.at[at], h_out.at[lax.rem(j, late), :, c], piece_sem.at[at]
        )

    @pl.loop(0, n_jobs)
    def _(j):
        e, slot = lax.rem(j, late), lax.rem(j, slots)
        for copy in fetches(j):
            copy.wait()
        size = (begin(e, 4) + STEP - 1) // STEP

        @pl.when(size == 0)
        def _():
            packed[...] = jnp.zeros_like(packed)

        for v in range(1, 5):

            @pl.when(size == v)
            def _(v=v):
                m = v * STEP
                first = pl.multiple_of(e * 4 * STEP, 16)
                both = dot(z[pl.ds(first, m), :], ring[slot])
                packed[:m, :] = (silu(both[:, :block]) * both[:, block:]).astype(BF16)
                packed[m : m + STEP, :] = jnp.zeros((STEP, block), BF16)

        @pl.when(j + slots < n_jobs)
        def _():
            for copy in fetches(j + slots):
                copy.start()

        @pl.when(j >= 2)
        def _():
            put(j - 2).wait()

        for k in range(4):
            piece[lax.rem(j, 2), k * STEP : (k + 1) * STEP, :] = packed[pl.ds(begin(e, k), STEP), :]
        put(j).start()

    put(jnp.int32(n_jobs - 2)).wait()
    put(jnp.int32(n_jobs - 1)).wait()


def up(meta, code, x0, xs, w_gate, w_up, block):
    experts, depth, ff = w_gate.shape
    late = experts - EARLY
    hbm, dma = pl.BlockSpec(memory_space=pl.ANY), pltpu.SemaphoreType.DMA
    return pl.pallas_call(
        up_kernel,
        in_specs=[
            pl.BlockSpec(memory_space=pltpu.SMEM),
            pl.BlockSpec(memory_space=pltpu.VMEM),
            hbm, hbm, hbm, hbm,
        ],
        out_specs=hbm,
        scratch_shapes=[
            pltpu.VMEM(((4 * late + 1) * STEP, depth), BF16),
            pltpu.VMEM((2, 4, 256, 1024), BF16),
            pltpu.VMEM((4, depth, 2 * block), BF16),
            pltpu.VMEM((5 * STEP, block), BF16),
            pltpu.VMEM((2, 4 * STEP, block), BF16),
            dma((2, 2)), dma((4, 2)), dma((2,)),
        ],
        out_shape=jax.ShapeDtypeStruct((late, 4 * STEP, ff), BF16),
        compiler_params=pltpu.CompilerParams(vmem_limit_bytes=VMEM),
        cost_estimate=pl.CostEstimate(
            flops=late * 300 * depth * ff * 4,
            bytes_accessed=late * depth * ff * 4,
            transcendentals=0,
        ),
        name="up",
    )(meta, code, x0, xs, w_gate, w_up)


def finish_kernel(
    chunks, code, gate, early, late, wd, shared, y,
    h, wt, stack, own, far, near, near_got, out, out_got,
    sem, near_send, near_recv, out_send, out_recv,
):
    experts, block = wd.shape[0], wd.shape[2]
    i = pl.program_id(0)
    me = lax.axis_index("ep")
    partner, across = me + 1 - 2 * lax.rem(me, 2), lax.rem(me + 2, 4)

    def remote(src, dst, send, recv, peer):
        return pltpu.make_async_remote_copy(
            src, dst, send, recv, device_id={"ep": peer}, device_id_type=pl.DeviceIdType.MESH
        )

    def to_partner(j):
        return remote(
            near.at[lax.rem(j, 2)], near_got.at[j], near_send.at[lax.rem(j, 2)], near_recv.at[j],
            partner,
        )

    def to_across(j):
        return remote(
            out.at[lax.rem(j, 2)], out_got.at[j], out_send.at[lax.rem(j, 2)], out_recv.at[j],
            across,
        )

    def load(e):
        src = early.at[e] if e < EARLY else late.at[e - EARLY]
        return pltpu.make_async_copy(src, h.at[e], sem.at[e])

    @pl.when(i == 0)
    def _():
        barrier = pltpu.get_barrier_semaphore()
        for peer in (partner, across):
            pl.semaphore_signal(
                barrier, inc=1, device_id={"ep": peer}, device_id_type=pl.DeviceIdType.MESH
            )
        for e in range(experts):
            load(e).start()
        stack[...] = jnp.zeros_like(stack)
        rows = lax.broadcasted_iota(jnp.int32, (STEP, 256), 0).astype(F32)
        for k in range(4):
            parts = [
                jnp.where(rows == code[e, k : k + 1, :], gate[e, k : k + 1, :], 0.0)
                for e in range(experts)
            ]
            parts.append(jnp.zeros((stack.shape[1] - experts * STEP, 256), F32))
            wt[k] = jnp.concatenate(parts, 0).T.astype(BF16)
        for e in range(experts // 2):
            load(e).wait()
        pl.semaphore_wait(barrier, 2)

    @pl.when(i >= 3)
    def _():
        j = i - 3
        to_across(j).wait_recv()
        total = own[lax.rem(j, 4)] + near_got[j, 0].astype(F32) + out_got[j].astype(F32)
        y[...] = (total + shared[...]).astype(BF16)

    def make(e):
        made = dot(h[e], wd[e]).astype(BF16)
        for k in range(4):
            stack[k, e * STEP : (e + 1) * STEP, :] = made[k * STEP : (k + 1) * STEP, :]

    half = experts // 2

    @pl.when(i < chunks)
    def _():
        for e in range(half):
            make(e)

    @pl.when((i >= 1) & (i <= chunks))
    def _():
        j = i - 1

        @pl.when(j >= 2)
        def _():
            to_across(j - 2).wait_send()

        to_partner(j).wait_recv()
        out[lax.rem(j, 2)] = (far[...] + near_got[j, 1].astype(F32)).astype(BF16)
        to_across(j).start()

    @pl.when(i == 0)
    def _():
        for e in range(half, experts):
            load(e).wait()

    @pl.when(i < chunks)
    def _():
        for e in range(half, experts):
            make(e)

        @pl.when(i >= 2)
        def _():
            to_partner(i - 2).wait_send()

        slot = lax.rem(i, 2)
        near[slot, 1] = dot(wt[3], stack[3]).astype(BF16)
        near[slot, 0] = dot(wt[1], stack[1]).astype(BF16)
        far[...] = dot(wt[2], stack[2])
        to_partner(i).start()
        own[lax.rem(i, 4)] = dot(wt[0], stack[0])

    @pl.when(i == chunks + 2)
    def _():
        for j in (chunks - 2, chunks - 1):
            to_partner(j).wait_send()
            to_across(j).wait_send()


def finish(code, gate, early, late, w_down, shared, block):
    experts, ff, d = w_down.shape
    chunks = d // block
    once = pl.Buffered(1)
    small = pl.BlockSpec((experts, 4, 256), lambda i: (0, 0, 0), pipeline_mode=once)
    result = pl.BlockSpec((256, block), lambda i: (0, jnp.maximum(i - 3, 0)))
    depth = -(-experts * STEP // 256) * 256
    dma = pltpu.SemaphoreType.DMA
    return pl.pallas_call(
        functools.partial(finish_kernel, chunks),
        grid=(chunks + 3,),
        in_specs=[
            small,
            small,
            pl.BlockSpec(memory_space=pl.ANY),
            pl.BlockSpec(memory_space=pl.ANY),
            pl.BlockSpec((experts, ff, block), lambda i: (0, 0, jnp.minimum(i, chunks - 1))),
            result,
        ],
        out_specs=result,
        scratch_shapes=[
            pltpu.VMEM((experts, 4 * STEP, ff), BF16),
            pltpu.VMEM((4, 256, depth), BF16),
            pltpu.VMEM((4, depth, block), BF16),
            pltpu.VMEM((4, 256, block), F32),
            pltpu.VMEM((256, block), F32),
            pltpu.VMEM((2, 2, 256, block), BF16),
            pltpu.VMEM((chunks, 2, 256, block), BF16),
            pltpu.VMEM((2, 256, block), BF16),
            pltpu.VMEM((chunks, 256, block), BF16),
            dma((experts,)),
            dma((2,)),
            dma((chunks,)),
            dma((2,)),
            dma((chunks,)),
        ],
        out_shape=jax.ShapeDtypeStruct((256, d), BF16),
        compiler_params=pltpu.CompilerParams(
            collective_id=1,
            has_side_effects=True,
            vmem_limit_bytes=VMEM,
            dimension_semantics=("arbitrary",),
        ),
        name="finish",
    )(code, gate, early, late, w_down, shared)


def layer(x, expert, slot, gate, w_gate, w_up, w_down, s_gate, s_up, s_down):
    local = w_gate.shape[0]
    x, expert, slot, gate = x[0, 0], expert[0, 0], slot[0, 0], gate[0, 0]
    xs, code, weight, early, shared = arrive(
        x, expert, slot, gate, w_gate, w_up, s_gate, s_up, s_down
    )
    used = (jnp.max(code, -1).astype(jnp.int32) + 16) // 16 * 16
    starts = [jnp.zeros_like(used[:, 0])]
    for k in range(4):
        starts.append(starts[-1] + used[:, k])
    meta = jnp.stack(starts + starts[:3], 1).reshape(-1)

    late = up(meta, code, x, xs, w_gate, w_up, 256)
    return finish(code, weight, early, late, w_down, shared, 512)[None, None]


def solution(mesh):
    rows, whole = P("dp", "ep"), P()
    return jax.shard_map(
        layer,
        mesh=mesh,
        in_specs=(rows,) * 4 + (P("ep"),) * 3 + (whole,) * 3,
        out_specs=rows,
        check_vma=False,
    )
```
